128 devices in a mesh: rows: 128 (over x, z, y, core).
Axes of the slice: x: 4, y: 4, z: 4, core: 2. Of those that a mesh axis runs over, the one named last changes fastest.
Arguments:
- history: float32 [32, 2048, 4096], P(None, 'rows'), may hold values from 0.2 to 1.8, as said below
- source: float32 [2048, 4096], P('rows'), may hold values from 0.5 to 2, as said below
- diffusivity: float32 [2048, 4096], P('rows'), may hold values from 0.5 to 2, as said below
- target: float32 [2048, 4096], P('rows'), may hold values from -0.5 to 2.5, as said below
Outputs:
- update: float32 [2048, 4096], P('rows')
- totals: float32 [2], replicated
The draws below stay inside these ranges and needn't reach their ends.
Inputs may be any that keep to these rules, and one draw needn't show every extreme that they name: `history`: every level is a field between 0.2 and 1.8, smooth with a small cell-by-cell variation. `source`: a positive field between 0.5 and 2. `diffusivity`: a positive field between 0.5 and 2, smooth with a small cell-by-cell variation. `target`: a field between -0.5 and 2.5, smooth with a small cell-by-cell variation.
All inputs are finite; a program needn't handle non-finite values.
Results may differ from the reference program's by a relative error of at most 0.0003.
Values sent between devices are 32-bit elements; how exact they have to be, the bound alone decides.
No kernel may reach another device: no remote copies, remote signals or barrier semaphores. Data moves between devices by JAX's collectives and lax.ppermute only.
A program may use at most 128 MiB of HBM per device.

```python
import math
import jax
import jax.numpy as jnp
from jax import lax

NY = 4096
LEVELS = 32
STIFF = 1024
NX = 2048


def smooth_pattern(base_key, row_count, col_count):
    subkeys = jax.random.split(base_key, 6)
    mode_count = 8
    two_pi = 2.0 * math.pi
    freq_rows = jax.random.uniform(subkeys[0], (mode_count,), jnp.float32, 0.5, 3.0)
    freq_cols = jax.random.uniform(subkeys[1], (mode_count,), jnp.float32, 0.5, 3.0)
    phase_rows = jax.random.uniform(subkeys[2], (mode_count,), jnp.float32, 0.0, two_pi)
    phase_cols = jax.random.uniform(subkeys[3], (mode_count,), jnp.float32, 0.0, two_pi)
    amplitude = 0.6 * jax.random.normal(subkeys[4], (mode_count,), jnp.float32)
    pos_rows = jnp.arange(row_count, dtype=jnp.float32) / row_count
    pos_cols = jnp.arange(col_count, dtype=jnp.float32) / col_count
    wave_rows = jnp.cos(two_pi * freq_rows[:, None] * pos_rows[None, :] + phase_rows[:, None])
    wave_cols = jnp.cos(two_pi * freq_cols[:, None] * pos_cols[None, :] + phase_cols[:, None])
    pattern = jnp.dot((amplitude[:, None] * wave_rows).T, wave_cols)
    jitter = 0.15 * jax.random.normal(subkeys[5], (row_count, col_count), jnp.float32)
    return jnp.tanh(pattern + jitter)


def banded_pattern(base_key, row_count, col_count):
    subkeys = jax.random.split(base_key, 6)
    two_pi = 2.0 * math.pi
    smooth_part = smooth_pattern(subkeys[0], row_count, col_count)
    column_noise = jax.random.uniform(subkeys[1], (col_count,), jnp.float32, -1.0, 1.0)
    row_noise = jax.random.uniform(subkeys[2], (row_count,), jnp.float32, -1.0, 1.0)
    phases = jax.random.uniform(subkeys[3], (2,), jnp.float32, 0.0, two_pi)
    pos_rows = jnp.arange(row_count, dtype=jnp.float32) / row_count
    pos_cols = jnp.arange(col_count, dtype=jnp.float32) / col_count
    column_mod = 0.75 + 0.25 * jnp.cos(two_pi * 1.5 * pos_rows + phases[0])
    row_mod = 0.75 + 0.25 * jnp.cos(two_pi * 1.5 * pos_cols + phases[1])
    jitter = 0.2 * jax.random.normal(subkeys[4], (row_count, col_count), jnp.float32)
    mixed = 0.5 * smooth_part + 1.3 * column_noise[None, :] * column_mod[:, None] + 1.3 * row_noise[:, None] * row_mod[None, :] + jitter
    return jnp.tanh(mixed)


def draw_history(key, part):
    level_keys = jax.random.split(jax.random.fold_in(key, 11), LEVELS)
    levels = lax.map(lambda one_key: smooth_pattern(one_key, NX, NY), level_keys)
    return 1.0 + 0.8 * levels


def draw_source(key, part):
    return 1.25 + 0.75 * banded_pattern(jax.random.fold_in(key, 23), NX, NY)


def draw_diffusivity(key, part):
    return jnp.exp(0.69 * smooth_pattern(jax.random.fold_in(key, 37), NX, NY))


def draw_target(key, part):
    return 1.0 + 1.5 * smooth_pattern(jax.random.fold_in(key, 41), NX, NY)


def setup_inputs(seed: int = 0) -> dict:
    arg_keys = jax.random.split(jax.random.key(seed), 5)
    return {
        "history": draw_history(jax.random.fold_in(arg_keys[4], 71), 0),
        "source": draw_source(jax.random.fold_in(arg_keys[4], 71), 0),
        "diffusivity": draw_diffusivity(jax.random.fold_in(arg_keys[4], 71), 0),
        "target": draw_target(jax.random.fold_in(arg_keys[4], 71), 0),
    }


frac_order = 0.6


def memory_weights(levels):
    moments = jnp.arange(levels + 1, dtype=jnp.float32)
    powered = moments ** (1.0 - frac_order)
    decay_terms = powered[1:] - powered[:-1]
    padding = jnp.zeros((1,), jnp.float32)
    return jnp.concatenate([decay_terms[1:], padding]) - jnp.concatenate([padding, decay_terms[1:]])


def line_bands(conduct):
    count_rows = conduct.shape[0]
    position = lax.broadcasted_iota(jnp.int32, conduct.shape, 0)
    coupling = -float(STIFF) * conduct
    sub_diag = jnp.where(position == 0, 0.0, coupling)
    sup_diag = jnp.where(position == count_rows - 1, 0.0, coupling)
    main_diag = 1.0 + 2.0 * float(STIFF) * conduct
    return sub_diag, main_diag, sup_diag


def thomas_solve(sub_diag, main_diag, sup_diag, right_side):
    def forward_pass(state_now, entries):
        ratio_prev, value_prev = state_now
        sub_now, main_now, sup_now, right_now = entries
        pivot_now = main_now - sub_now * ratio_prev
        ratio_new = sup_now / pivot_now
        value_new = (right_now - sub_now * value_prev) / pivot_now
        return (ratio_new, value_new), (ratio_new, value_new)

    zeros_row = jnp.zeros_like(right_side[0])
    _, (ratios, values_fwd) = lax.scan(forward_pass, (zeros_row, zeros_row), (sub_diag, main_diag, sup_diag, right_side))

    def backward_pass(later_value, entries):
        ratio_now, value_now = entries
        result_now = value_now - ratio_now * later_value
        return result_now, result_now

    _, solution = lax.scan(backward_pass, zeros_row, (ratios, values_fwd), reverse=True)
    return solution


def reference(history, source, diffusivity, target):
    weights = memory_weights(LEVELS)
    flat_hist = history.reshape(LEVELS, NX * NY)
    memory = jnp.dot(weights, flat_hist, precision=lax.Precision.HIGHEST).reshape(NX, NY)
    driven = history[0] - memory + source
    sub_x, main_x, sup_x = line_bands(diffusivity.T)
    swept = thomas_solve(sub_x, main_x, sup_x, driven.T).T
    sub_y, main_y, sup_y = line_bands(diffusivity)
    update = thomas_solve(sub_y, main_y, sup_y, swept)
    cell_count = float(NX * NY)
    totals = jnp.stack([jnp.sum(update) / cell_count, jnp.sum((update - target) ** 2) / cell_count])
    return update, totals
```

```python
import jax
import jax.numpy as jnp
import numpy as np
from jax import lax
from jax.experimental import pallas as pl
from jax.experimental.pallas import tpu as pltpu
from jax.sharding import PartitionSpec as P

STIFF = 1024.0
ORDER = 0.6
AXIS = "rows"
LANES = 128
SUB = 8
LEVELS = 32
ROWS = 16
NY = 4096
TILES = NY // LANES
HALVES = ROWS // SUB
VREGS = HALVES * TILES
BLOCKS = 128
INNER = ROWS - 1
CHUNKS = 8
CHUNK_TILES = TILES // CHUNKS
STEPS = 12
F32 = jnp.float32


def history_weights():
    moments = np.arange(LEVELS + 1, dtype=np.float64) ** (1.0 - ORDER)
    b = moments[1:] - moments[:-1]
    w = np.concatenate([b[1:], [0.0]]) - np.concatenate([[0.0], b[1:]])
    scale = -w
    scale[0] = 1.0 - w[0]
    return [float(v) for v in scale.astype(np.float32)]


def tile(h, t):
    return pl.ds((h * TILES + t % TILES) * SUB, SUB)


def line(r):
    return pl.ds((r // SUB) * TILES * SUB + r % SUB, TILES, stride=SUB)


def wide(r):
    return pl.ds(r * TILES, TILES)


def shifted(values, stride, lane):
    if stride >= LANES:
        hop = stride // LANES
        low = [values[(t - hop) % TILES] for t in range(TILES)]
        high = [values[(t + hop) % TILES] for t in range(TILES)]
        return low, high
    down = [pltpu.roll(v, stride, 1) for v in values]
    up = [pltpu.roll(v, LANES - stride, 1) for v in values]
    low = [jnp.where(lane < stride, down[t - 1], down[t]) for t in range(TILES)]
    high = [
        jnp.where(lane >= LANES - stride, up[(t + 1) % TILES], up[t]) for t in range(TILES)
    ]
    return low, high


def local_kernel(
    hist_hbm, src_hbm, dif_hbm, tgt_hbm,
    msg, part, above, below,
    hist, src, dif, tgt,
    alpha, beta, main, sub, sup, inv, rhs,
    dif_l, tgt_l, sw_l, gg, hh, rr, pp,
    sems,
):
    copies = [
        pltpu.make_async_copy(dif_hbm, dif, sems.at[0]),
        pltpu.make_async_copy(src_hbm, src, sems.at[1]),
    ]
    width = CHUNK_TILES * LANES
    for c in range(CHUNKS):
        cols = pl.ds(c * width, width)
        copies.append(
            pltpu.make_async_copy(
                hist_hbm.at[:, :, cols], hist.at[:, :, cols], sems.at[3 + c]
            )
        )
    copies.append(pltpu.make_async_copy(tgt_hbm, tgt, sems.at[2]))
    for copy in copies:
        copy.start()
    lane = lax.broadcasted_iota(jnp.int32, (SUB, LANES), 1)

    copies[0].wait()
    for h in range(HALVES):
        for t in range(TILES):
            c = STIFF * dif[h * SUB:(h + 1) * SUB, t * LANES:(t + 1) * LANES]
            dif_l[tile(h, t), :] = c
            m = 1.0 + 2.0 * c
            main[0, tile(h, t), :] = m
            inv[0, tile(h, t), :] = 1.0 / m
            sub[0, tile(h, t), :] = jnp.where(lane == 0, 0.0, c) if t == 0 else c
            sup[0, tile(h, t), :] = jnp.where(lane == LANES - 1, 0.0, c) if t == TILES - 1 else c

    g = h_ = None
    for r in range(ROWS):
        c = dif_l[line(r), :]
        if r == 0:
            q = 1.0 / (1.0 + 2.0 * c)
            g = c * q
            h_ = g
        else:
            q = 1.0 / (1.0 + 2.0 * c - c * g)
            g = c * q
            h_ = g * h_
        rr[wide(r), :] = q
        gg[wide(r), :] = g
        hh[wide(r), :] = h_
    a = hh[wide(INNER - 1), :]
    b = gg[wide(INNER - 1), :]
    zero = jnp.zeros((TILES, LANES), F32)
    sum_a = sum_b = sum_aa = sum_ab = sum_bb = zero
    for r in reversed(range(INNER)):
        if r < INNER - 1:
            g = gg[wide(r), :]
            a = hh[wide(r), :] + g * a
            b = g * b
        above[wide(r), :] = a
        below[wide(r), :] = b
        sum_a = sum_a + a
        sum_b = sum_b + b
        sum_aa = sum_aa + a * a
        sum_ab = sum_ab + a * b
        sum_bb = sum_bb + b * b
    def send(group, four):
        stacked = jnp.concatenate(four, axis=0)
        msg[pl.ds(group, BLOCKS, stride=4), :] = stacked.T

    send(0, [a, b, hh[wide(INNER), :], gg[wide(INNER), :]])
    send(1, [sum_a, sum_b + 1.0, sum_aa, sum_ab])

    for k in range(STEPS):
        stride = 1 << k
        now = k % 2
        nxt = 1 - now
        for h in range(HALVES):
            e = [sub[now, tile(h, t), :] for t in range(TILES)]
            f = [sup[now, tile(h, t), :] for t in range(TILES)]
            v = [inv[now, tile(h, t), :] for t in range(TILES)]
            e_low, e_high = shifted(e, stride, lane)
            f_low, f_high = shifted(f, stride, lane)
            v_low, v_high = shifted(v, stride, lane)
            for t in range(TILES):
                al = e[t] * v_low[t]
                be = f[t] * v_high[t]
                m = main[now, tile(h, t), :] - al * f_low[t] - be * e_high[t]
                alpha[k, tile(h, t), :] = al
                beta[k, tile(h, t), :] = be
                if k < STEPS - 1:
                    main[nxt, tile(h, t), :] = m
                    sub[nxt, tile(h, t), :] = al * e_low[t]
                    sup[nxt, tile(h, t), :] = be * f_high[t]
                inv[nxt, tile(h, t), :] = 1.0 / m

    scale = history_weights()
    copies[1].wait()
    for c in range(CHUNKS):
        copies[2 + c].wait()
        for h in range(HALVES):
            rows = slice(h * SUB, (h + 1) * SUB)
            for t in range(c * CHUNK_TILES, (c + 1) * CHUNK_TILES):
                cols = slice(t * LANES, (t + 1) * LANES)
                acc = src[rows, cols]
                for k in range(LEVELS):
                    acc = acc + scale[k] * hist[k, rows, cols]
                rhs[0, tile(h, t), :] = acc

    for k in range(STEPS):
        now = k % 2
        nxt = 1 - now
        for h in range(HALVES):
            d = [rhs[now, tile(h, t), :] for t in range(TILES)]
            low, high = shifted(d, 1 << k, lane)
            for t in range(TILES):
                n = (
                    d[t]
                    + alpha[k, tile(h, t), :] * low[t]
                    + beta[k, tile(h, t), :] * high[t]
                )
                if k < STEPS - 1:
                    rhs[nxt, tile(h, t), :] = n
                else:
                    sw_l[tile(h, t), :] = n * inv[nxt, tile(h, t), :]

    copies[2 + CHUNKS].wait()
    for h in range(HALVES):
        for t in range(TILES):
            tgt_l[tile(h, t), :] = tgt[h * SUB:(h + 1) * SUB, t * LANES:(t + 1) * LANES]
    p = None
    for r in range(ROWS):
        s = rr[wide(r), :] * sw_l[line(r), :]
        p = s if r == 0 else s + gg[wide(r), :] * p
        pp[wide(r), :] = p
    tip = p
    d = tgt_l[line(INNER), :]
    sum_dd = d * d
    sum_db = -d
    sum_da = zero
    sum_p = zero
    p = pp[wide(INNER - 1), :]
    for r in reversed(range(INNER)):
        if r < INNER - 1:
            p = pp[wide(r), :] + gg[wide(r), :] * p
        part[wide(r), :] = p
        a = above[wide(r), :]
        b = below[wide(r), :]
        d = p - tgt_l[line(r), :]
        sum_p = sum_p + p
        sum_dd = sum_dd + d * d
        sum_da = sum_da + d * a
        sum_db = sum_db + d * b
    send(2, [p, tip, sum_p, sum_dd])
    send(3, [sum_da, sum_db, sum_bb + 1.0, zero])


def reduced_kernel(got, back):
    groups = [got[pl.ds(g, BLOCKS, stride=4), :].T for g in range(4)]
    q = [groups[i // 4][(i % 4) * TILES:(i % 4 + 1) * TILES] for i in range(15)]
    (a0, b0, u, v, sum_a, sum_b, sum_aa, sum_ab, p0, w, sum_p, sum_dd, sum_da, sum_db, sum_bb) = q
    lane = lax.broadcasted_iota(jnp.int32, (TILES, LANES), 1)
    u = jnp.where(lane == 0, 0.0, u)
    v = jnp.where(lane == BLOCKS - 1, 0.0, v)

    def low(x, s):
        return pltpu.roll(x, s, 1)

    def high(x, s):
        return pltpu.roll(x, LANES - s, 1)

    r = 1.0 / (1.0 - v * high(a0, 1))
    e = u * r
    f = v * high(b0, 1) * r
    d = (w + v * high(p0, 1)) * r
    s = 1
    while s < BLOCKS:
        r = 1.0 / (1.0 - e * low(f, s) - f * high(e, s))
        d = (d + e * low(d, s) + f * high(d, s)) * r
        if 2 * s < BLOCKS:
            e, f = e * low(e, s) * r, f * high(f, s) * r
        s *= 2
    z = d
    x = jnp.where(lane == 0, 0.0, low(z, 1))
    mass = sum_p + sum_a * x + sum_b * z
    error = (
        sum_dd
        + 2.0 * (sum_da * x + sum_db * z + sum_ab * x * z)
        + sum_aa * x * x
        + sum_bb * z * z
    )

    def total(y):
        y = jnp.sum(jnp.sum(y, axis=0, keepdims=True), axis=1, keepdims=True)
        return jnp.broadcast_to(y, (SUB, LANES))

    rest = jnp.zeros((LANES - 2 * TILES - 2 * SUB, LANES), F32)
    back[...] = jnp.concatenate([z, x, total(mass), total(error), rest], axis=0).T


def final_kernel(got, part, above, below, update, totals, lines):
    t = got[...].T
    z = t[:TILES]
    x = t[TILES:2 * TILES]
    scale = 1.0 / (BLOCKS * ROWS * NY)
    totals[0] = jnp.sum(t[2 * TILES:2 * TILES + 1]) * scale
    totals[1] = jnp.sum(t[2 * TILES + SUB:2 * TILES + SUB + 1]) * scale
    for r in range(INNER):
        lines[line(r), :] = part[wide(r), :] + above[wide(r), :] * x + below[wide(r), :] * z
    lines[line(INNER), :] = z
    for h in range(HALVES):
        for i in range(TILES):
            update[h * SUB:(h + 1) * SUB, i * LANES:(i + 1) * LANES] = lines[tile(h, i), :]


def body(history, source, diffusivity, target):
    anywhere = pl.BlockSpec(memory_space=pl.ANY)
    vmem = pl.BlockSpec(memory_space=pltpu.VMEM)
    shape = jax.ShapeDtypeStruct
    block = pltpu.VMEM((ROWS, NY), F32)
    tiles = pltpu.VMEM((VREGS * SUB, LANES), F32)
    pair = pltpu.VMEM((2, VREGS * SUB, LANES), F32)
    lines = INNER * TILES
    params = pltpu.CompilerParams(vmem_limit_bytes=48 * 1024 * 1024)
    msg, part, above, below = pl.pallas_call(
        local_kernel,
        name="local",
        out_shape=[shape((4 * BLOCKS, LANES), F32)] + [shape((lines, LANES), F32)] * 3,
        in_specs=[anywhere] * 4,
        out_specs=[vmem] * 4,
        scratch_shapes=[
            pltpu.VMEM((LEVELS, ROWS, NY), F32), block, block, block,
            pltpu.VMEM((STEPS, VREGS * SUB, LANES), F32),
            pltpu.VMEM((STEPS, VREGS * SUB, LANES), F32),
            pair, pair, pair, pair, pair,
            tiles, tiles, tiles, tiles, tiles, tiles, tiles,
            pltpu.SemaphoreType.DMA((3 + CHUNKS,)),
        ],
        compiler_params=params,
    )(history, source, diffusivity, target)
    got = lax.all_to_all(
        msg.reshape(BLOCKS, 4, LANES), AXIS, split_axis=0, concat_axis=0, tiled=True
    ).reshape(4 * BLOCKS, LANES)
    back = pl.pallas_call(
        reduced_kernel,
        name="reduced",
        out_shape=shape((BLOCKS, LANES), F32),
        in_specs=[vmem],
        out_specs=vmem,
        compiler_params=params,
    )(got)
    solved = lax.all_to_all(back, AXIS, split_axis=0, concat_axis=0, tiled=True)
    return pl.pallas_call(
        final_kernel,
        name="final",
        out_shape=[shape((ROWS, NY), F32), shape((2,), F32)],
        in_specs=[vmem] * 4,
        out_specs=[vmem, pl.BlockSpec(memory_space=pltpu.SMEM)],
        scratch_shapes=[tiles],
        compiler_params=params,
    )(solved, part, above, below)


def solution(mesh):
    return jax.shard_map(
        body,
        mesh=mesh,
        in_specs=(P(None, AXIS, None), P(AXIS, None), P(AXIS, None), P(AXIS, None)),
        out_specs=(P(AXIS, None), P()),
        check_vma=False,
    )
```

```python
import jax
import jax.numpy as jnp
import numpy as np
from jax import lax
from jax.experimental import pallas as pl
from jax.experimental.pallas import tpu as pltpu
from jax.sharding import PartitionSpec as P

STIFF = 1024.0
ORDER = 0.6
AXIS = "rows"
LANES = 128
SUB = 8
LEVELS = 32
ROWS = 16
NY = 4096
TILES = NY // LANES
HALVES = ROWS // SUB
VREGS = HALVES * TILES
BLOCKS = 128
INNER = ROWS - 1
CHUNKS = 8
CHUNK_TILES = TILES // CHUNKS
STEPS = 12
F32 = jnp.float32


def history_weights():
    moments = np.arange(LEVELS + 1, dtype=np.float64) ** (1.0 - ORDER)
    b = moments[1:] - moments[:-1]
    w = np.concatenate([b[1:], [0.0]]) - np.concatenate([[0.0], b[1:]])
    scale = -w
    scale[0] = 1.0 - w[0]
    return [float(v) for v in scale.astype(np.float32)]


def tile(h, t):
    return pl.ds((h * TILES + t % TILES) * SUB, SUB)


def line(r):
    return pl.ds((r // SUB) * TILES * SUB + r % SUB, TILES, stride=SUB)


def wide(r):
    return pl.ds(r * TILES, TILES)


def shifted(values, stride, lane):
    if stride >= LANES:
        hop = stride // LANES
        low = [values[(t - hop) % TILES] for t in range(TILES)]
        high = [values[(t + hop) % TILES] for t in range(TILES)]
        return low, high
    down = [pltpu.roll(v, stride, 1) for v in values]
    up = [pltpu.roll(v, LANES - stride, 1) for v in values]
    low = [jnp.where(lane < stride, down[t - 1], down[t]) for t in range(TILES)]
    high = [
        jnp.where(lane >= LANES - stride, up[(t + 1) % TILES], up[t]) for t in range(TILES)
    ]
    return low, high


def local_kernel(
    hist_hbm, src_hbm, dif_hbm, tgt_hbm,
    msg, part, above, below,
    hist, src, dif, tgt,
    alpha, beta, main, sub, sup, inv, rhs,
    dif_l, tgt_l, sw_l, gg, hh, rr, pp,
    sems,
):
    copies = [
        pltpu.make_async_copy(dif_hbm, dif, sems.at[0]),
        pltpu.make_async_copy(src_hbm, src, sems.at[1]),
    ]
    width = CHUNK_TILES * LANES
    for c in range(CHUNKS):
        cols = pl.ds(c * width, width)
        copies.append(
            pltpu.make_async_copy(
                hist_hbm.at[:, :, cols], hist.at[:, :, cols], sems.at[3 + c]
            )
        )
    copies.append(pltpu.make_async_copy(tgt_hbm, tgt, sems.at[2]))
    for copy in copies:
        copy.start()
    lane = lax.broadcasted_iota(jnp.int32, (SUB, LANES), 1)

    copies[0].wait()
    for h in range(HALVES):
        for t in range(TILES):
            c = STIFF * dif[h * SUB:(h + 1) * SUB, t * LANES:(t + 1) * LANES]
            dif_l[tile(h, t), :] = c
            m = 1.0 + 2.0 * c
            main[0, tile(h, t), :] = m
            inv[0, tile(h, t), :] = 1.0 / m
            sub[0, tile(h, t), :] = jnp.where(lane == 0, 0.0, c) if t == 0 else c
            sup[0, tile(h, t), :] = jnp.where(lane == LANES - 1, 0.0, c) if t == TILES - 1 else c

    g = h_ = None
    for r in range(ROWS):
        c = dif_l[line(r), :]
        if r == 0:
            q = 1.0 / (1.0 + 2.0 * c)
            g = c * q
            h_ = g
        else:
            q = 1.0 / (1.0 + 2.0 * c - c * g)
            g = c * q
            h_ = g * h_
        rr[wide(r), :] = q
        gg[wide(r), :] = g
        hh[wide(r), :] = h_
    a = hh[wide(INNER - 1), :]
    b = gg[wide(INNER - 1), :]
    zero = jnp.zeros((TILES, LANES), F32)
    sum_a = sum_b = sum_aa = sum_ab = sum_bb = zero
    for r in reversed(range(INNER)):
        if r < INNER - 1:
            g = gg[wide(r), :]
            a = hh[wide(r), :] + g * a
            b = g * b
        above[wide(r), :] = a
        below[wide(r), :] = b
        sum_a = sum_a + a
        sum_b = sum_b + b
        sum_aa = sum_aa + a * a
        sum_ab = sum_ab + a * b
        sum_bb = sum_bb + b * b
    def send(group, four):
        stacked = jnp.concatenate(four, axis=0)
        msg[pl.ds(group, BLOCKS, stride=4), :] = stacked.T

    send(0, [a, b, hh[wide(INNER), :], gg[wide(INNER), :]])
    send(1, [sum_a, sum_b + 1.0, sum_aa, sum_ab])

    for k in range(STEPS):
        stride = 1 << k
        now = k % 2
        nxt = 1 - now
        for h in range(HALVES):
            e = [sub[now, tile(h, t), :] for t in range(TILES)]
            f = [sup[now, tile(h, t), :] for t in range(TILES)]
            v = [inv[now, tile(h, t), :] for t in range(TILES)]
            e_low, e_high = shifted(e, stride, lane)
            f_low, f_high = shifted(f, stride, lane)
            v_low, v_high = shifted(v, stride, lane)
            for t in range(TILES):
                al = e[t] * v_low[t]
                be = f[t] * v_high[t]
                m = main[now, tile(h, t), :] - al * f_low[t] - be * e_high[t]
                alpha[k, tile(h, t), :] = al
                beta[k, tile(h, t), :] = be
                if k < STEPS - 1:
                    main[nxt, tile(h, t), :] = m
                    sub[nxt, tile(h, t), :] = al * e_low[t]
                    sup[nxt, tile(h, t), :] = be * f_high[t]
                inv[nxt, tile(h, t), :] = 1.0 / m

    scale = history_weights()
    copies[1].wait()
    for c in range(CHUNKS):
        copies[2 + c].wait()
        for h in range(HALVES):
            rows = slice(h * SUB, (h + 1) * SUB)
            for t in range(c * CHUNK_TILES, (c + 1) * CHUNK_TILES):
                cols = slice(t * LANES, (t + 1) * LANES)
                acc = src[rows, cols]
                for k in range(LEVELS):
                    acc = acc + scale[k] * hist[k, rows, cols]
                rhs[0, tile(h, t), :] = acc

    for k in range(STEPS):
        now = k % 2
        nxt = 1 - now
        for h in range(HALVES):
            d = [rhs[now, tile(h, t), :] for t in range(TILES)]
            low, high = shifted(d, 1 << k, lane)
            for t in range(TILES):
                n = (
                    d[t]
                    + alpha[k, tile(h, t), :] * low[t]
                    + beta[k, tile(h, t), :] * high[t]
                )
                if k < STEPS - 1:
                    rhs[nxt, tile(h, t), :] = n
                else:
                    sw_l[tile(h, t), :] = n * inv[nxt, tile(h, t), :]

    copies[2 + CHUNKS].wait()
    for h in range(HALVES):
        for t in range(TILES):
            tgt_l[tile(h, t), :] = tgt[h * SUB:(h + 1) * SUB, t * LANES:(t + 1) * LANES]
    p = None
    for r in range(ROWS):
        s = rr[wide(r), :] * sw_l[line(r), :]
        p = s if r == 0 else s + gg[wide(r), :] * p
        pp[wide(r), :] = p
    tip = p
    d = tgt_l[line(INNER), :]
    sum_dd = d * d
    sum_db = -d
    sum_da = zero
    sum_p = zero
    p = pp[wide(INNER - 1), :]
    for r in reversed(range(INNER)):
        if r < INNER - 1:
            p = pp[wide(r), :] + gg[wide(r), :] * p
        part[wide(r), :] = p
        a = above[wide(r), :]
        b = below[wide(r), :]
        d = p - tgt_l[line(r), :]
        sum_p = sum_p + p
        sum_dd = sum_dd + d * d
        sum_da = sum_da + d * a
        sum_db = sum_db + d * b
    send(2, [p, tip, sum_p, sum_dd])
    send(3, [sum_da, sum_db, sum_bb + 1.0, zero])


def reduced_kernel(got, back):
    groups = [got[pl.ds(g, BLOCKS, stride=4), :].T for g in range(4)]
    q = [groups[i // 4][(i % 4) * TILES:(i % 4 + 1) * TILES] for i in range(15)]
    (a0, b0, u, v, sum_a, sum_b, sum_aa, sum_ab, p0, w, sum_p, sum_dd, sum_da, sum_db, sum_bb) = q
    lane = lax.broadcasted_iota(jnp.int32, (TILES, LANES), 1)
    u = jnp.where(lane == 0, 0.0, u)
    v = jnp.where(lane == BLOCKS - 1, 0.0, v)

    def low(x, s):
        return pltpu.roll(x, s, 1)

    def high(x, s):
        return pltpu.roll(x, LANES - s, 1)

    r = 1.0 / (1.0 - v * high(a0, 1))
    e = u * r
    f = v * high(b0, 1) * r
    d = (w + v * high(p0, 1)) * r
    s = 1
    while s < BLOCKS:
        r = 1.0 / (1.0 - e * low(f, s) - f * high(e, s))
        d = (d + e * low(d, s) + f * high(d, s)) * r
        if 2 * s < BLOCKS:
            e, f = e * low(e, s) * r, f * high(f, s) * r
        s *= 2
    z = d
    x = jnp.where(lane == 0, 0.0, low(z, 1))
    mass = sum_p + sum_a * x + sum_b * z
    error = (
        sum_dd
        + 2.0 * (sum_da * x + sum_db * z + sum_ab * x * z)
        + sum_aa * x * x
        + sum_bb * z * z
    )

    def total(y):
        y = jnp.sum(jnp.sum(y, axis=0, keepdims=True), axis=1, keepdims=True)
        return jnp.broadcast_to(y, (SUB, LANES))

    rest = jnp.zeros((LANES - 2 * TILES - 2 * SUB, LANES), F32)
    back[...] = jnp.concatenate([z, x, total(mass), total(error), rest], axis=0).T


def final_kernel(got, part, above, below, update, totals, lines):
    t = got[...].T
    z = t[:TILES]
    x = t[TILES:2 * TILES]
    scale = 1.0 / (BLOCKS * ROWS * NY)
    totals[0] = jnp.sum(t[2 * TILES:2 * TILES + 1]) * scale
    totals[1] = jnp.sum(t[2 * TILES + SUB:2 * TILES + SUB + 1]) * scale
    for r in range(INNER):
        lines[line(r), :] = part[wide(r), :] + above[wide(r), :] * x + below[wide(r), :] * z
    lines[line(INNER), :] = z
    for h in range(HALVES):
        for i in range(TILES):
            update[h * SUB:(h + 1) * SUB, i * LANES:(i + 1) * LANES] = lines[tile(h, i), :]


def body(history, source, diffusivity, target):
    anywhere = pl.BlockSpec(memory_space=pltpu.HBM)
    vmem = pl.BlockSpec(memory_space=pltpu.VMEM)
    shape = jax.ShapeDtypeStruct
    block = pltpu.VMEM((ROWS, NY), F32)
    tiles = pltpu.VMEM((VREGS * SUB, LANES), F32)
    pair = pltpu.VMEM((2, VREGS * SUB, LANES), F32)
    lines = INNER * TILES
    params = pltpu.CompilerParams(vmem_limit_bytes=48 * 1024 * 1024)
    msg, part, above, below = pl.pallas_call(
        local_kernel,
        name="local",
        out_shape=[shape((4 * BLOCKS, LANES), F32)] + [shape((lines, LANES), F32)] * 3,
        in_specs=[anywhere] * 4,
        out_specs=[vmem] * 4,
        scratch_shapes=[
            pltpu.VMEM((LEVELS, ROWS, NY), F32), block, block, block,
            pltpu.VMEM((STEPS, VREGS * SUB, LANES), F32),
            pltpu.VMEM((STEPS, VREGS * SUB, LANES), F32),
            pair, pair, pair, pair, pair,
            tiles, tiles, tiles, tiles, tiles, tiles, tiles,
            pltpu.SemaphoreType.DMA((3 + CHUNKS,)),
        ],
        compiler_params=params,
    )(*(pltpu.with_memory_space_constraint(x, pltpu.HBM) for x in (history, source, diffusivity, target)))
    got = lax.all_to_all(
        msg.reshape(BLOCKS, 4, LANES), AXIS, split_axis=0, concat_axis=0, tiled=True
    ).reshape(4 * BLOCKS, LANES)
    back = pl.pallas_call(
        reduced_kernel,
        name="reduced",
        out_shape=shape((BLOCKS, LANES), F32),
        in_specs=[vmem],
        out_specs=vmem,
        compiler_params=params,
    )(got)
    solved = lax.all_to_all(back, AXIS, split_axis=0, concat_axis=0, tiled=True)
    return pl.pallas_call(
        final_kernel,
        name="final",
        out_shape=[shape((ROWS, NY), F32), shape((2,), F32)],
        in_specs=[vmem] * 4,
        out_specs=[vmem, pl.BlockSpec(memory_space=pltpu.SMEM)],
        scratch_shapes=[tiles],
        compiler_params=params,
    )(solved, part, above, below)


def solution(mesh):
    return jax.shard_map(
        body,
        mesh=mesh,
        in_specs=(P(None, AXIS, None), P(AXIS, None), P(AXIS, None), P(AXIS, None)),
        out_specs=(P(AXIS, None), P()),
        check_vma=False,
    )
```

```python
import jax
import jax.numpy as jnp
import numpy as np
from jax import lax
from jax.experimental import pallas as pl
from jax.experimental.pallas import tpu as pltpu
from jax.sharding import PartitionSpec as P

STIFF = 1024.0
ORDER = 0.6
AXIS = "rows"
LANES = 128
SUB = 8
LEVELS = 32
ROWS = 16
NY = 4096
TILES = NY // LANES
HALVES = ROWS // SUB
VREGS = HALVES * TILES
BLOCKS = 128
INNER = ROWS - 1
CHUNKS = 4
CHUNK_TILES = TILES // CHUNKS
STEPS = 12
F32 = jnp.float32


def history_weights():
    moments = np.arange(LEVELS + 1, dtype=np.float64) ** (1.0 - ORDER)
    b = moments[1:] - moments[:-1]
    w = np.concatenate([b[1:], [0.0]]) - np.concatenate([[0.0], b[1:]])
    scale = -w
    scale[0] = 1.0 - w[0]
    return [float(v) for v in scale.astype(np.float32)]


def tile(h, t):
    return pl.ds((h * TILES + t % TILES) * SUB, SUB)


def line(r):
    return pl.ds((r // SUB) * TILES * SUB + r % SUB, TILES, stride=SUB)


def wide(r):
    return pl.ds(r * TILES, TILES)


def neighbours(load, stride, lane):
    if stride >= LANES:
        hop = stride // LANES
        for t in range(TILES):
            yield load(t), load(t - hop), load(t + hop)
        return
    back = LANES - stride
    before = pltpu.roll(load(TILES - 1), stride, 1)
    first = pltpu.roll(load(0), back, 1)
    here = first
    for t in range(TILES):
        value = load(t)
        down = pltpu.roll(value, stride, 1)
        after = first if t == TILES - 1 else pltpu.roll(load(t + 1), back, 1)
        yield value, jnp.where(lane < stride, before, down), jnp.where(lane >= back, after, here)
        before, here = down, after


def local_kernel(
    hist_hbm, src_hbm, dif_hbm, tgt_hbm,
    msg, part, above, below,
    hist, src, dif, tgt,
    lower, upper, pivot, first, rhs,
    dif_l, tgt_l, sw_l, gg, hh, rr, pp,
    sems,
):
    copies = [
        pltpu.make_async_copy(dif_hbm, dif, sems.at[0]),
        pltpu.make_async_copy(src_hbm, src, sems.at[1]),
        pltpu.make_async_copy(tgt_hbm, tgt, sems.at[2]),
    ]
    width = CHUNK_TILES * LANES
    for h in range(HALVES):
        rows = pl.ds(h * SUB, SUB)
        for c in range(CHUNKS):
            cols = pl.ds(c * width, width)
            copies.append(
                pltpu.make_async_copy(
                    hist_hbm.at[:, rows, cols], hist.at[:, rows, cols], sems.at[len(copies)]
                )
            )
    for copy in copies:
        copy.start()
    lane = lax.broadcasted_iota(jnp.int32, (SUB, LANES), 1)

    copies[0].wait()
    for h in range(HALVES):
        for t in range(TILES):
            c = STIFF * dif[h * SUB:(h + 1) * SUB, t * LANES:(t + 1) * LANES]
            dif_l[tile(h, t), :] = c
            q = 1.0 / (1.0 + 2.0 * c)
            first[tile(h, t), :] = q
            c = c * q
            lower[0, tile(h, t), :] = jnp.where(lane == 0, 0.0, c) if t == 0 else c
            upper[0, tile(h, t), :] = jnp.where(lane == LANES - 1, 0.0, c) if t == TILES - 1 else c

    g = h_ = None
    for r in range(ROWS):
        c = dif_l[line(r), :]
        if r == 0:
            q = 1.0 / (1.0 + 2.0 * c)
            g = c * q
            h_ = g
        else:
            q = 1.0 / (1.0 + 2.0 * c - c * g)
            g = c * q
            h_ = g * h_
        rr[wide(r), :] = q
        gg[wide(r), :] = g
        hh[wide(r), :] = h_
    a = hh[wide(INNER - 1), :]
    b = gg[wide(INNER - 1), :]
    zero = jnp.zeros((TILES, LANES), F32)
    sum_a = sum_b = sum_aa = sum_ab = sum_bb = zero
    for r in reversed(range(INNER)):
        if r < INNER - 1:
            g = gg[wide(r), :]
            a = hh[wide(r), :] + g * a
            b = g * b
        above[wide(r), :] = a
        below[wide(r), :] = b
        sum_a = sum_a + a
        sum_b = sum_b + b
        sum_aa = sum_aa + a * a
        sum_ab = sum_ab + a * b
        sum_bb = sum_bb + b * b
    def send(group, four):
        stacked = jnp.concatenate(four, axis=0)
        msg[pl.ds(group, BLOCKS, stride=4), :] = stacked.T

    send(0, [a, b, hh[wide(INNER), :], gg[wide(INNER), :]])
    send(1, [sum_a, sum_b + 1.0, sum_aa, sum_ab])

    for k in range(STEPS):
        for h in range(HALVES):
            lows = neighbours(lambda t: lower[k, tile(h, t), :], 1 << k, lane)
            highs = neighbours(lambda t: upper[k, tile(h, t), :], 1 << k, lane)
            for t in range(TILES):
                e, e_low, e_high = next(lows)
                f, f_low, f_high = next(highs)
                q = 1.0 / (1.0 - e * f_low - f * e_high)
                pivot[k, tile(h, t), :] = q
                if k < STEPS - 1:
                    lower[k + 1, tile(h, t), :] = e * e_low * q
                    upper[k + 1, tile(h, t), :] = f * f_high * q

    scale = history_weights()
    copies[1].wait()
    copies[2].wait()
    for h in range(HALVES):
        rows = slice(h * SUB, (h + 1) * SUB)
        for t in range(TILES):
            tgt_l[tile(h, t), :] = tgt[rows, t * LANES:(t + 1) * LANES]
    for h in range(HALVES):
        rows = slice(h * SUB, (h + 1) * SUB)
        for c in range(CHUNKS):
            copies[3 + h * CHUNKS + c].wait()
            for t in range(c * CHUNK_TILES, (c + 1) * CHUNK_TILES):
                cols = slice(t * LANES, (t + 1) * LANES)
                acc = src[rows, cols]
                for k in range(LEVELS):
                    acc = acc + scale[k] * hist[k, rows, cols]
                rhs[0, tile(h, t), :] = acc * first[tile(h, t), :]
        for k in range(STEPS):
            now = k % 2
            values = neighbours(lambda t: rhs[now, tile(h, t), :], 1 << k, lane)
            for t in range(TILES):
                d, low, high = next(values)
                d = (
                    d + lower[k, tile(h, t), :] * low + upper[k, tile(h, t), :] * high
                ) * pivot[k, tile(h, t), :]
                if k < STEPS - 1:
                    rhs[1 - now, tile(h, t), :] = d
                else:
                    sw_l[tile(h, t), :] = d

    p = None
    for r in range(ROWS):
        s = rr[wide(r), :] * sw_l[line(r), :]
        p = s if r == 0 else s + gg[wide(r), :] * p
        pp[wide(r), :] = p
    tip = p
    d = tgt_l[line(INNER), :]
    sum_dd = d * d
    sum_db = -d
    sum_da = zero
    sum_p = zero
    p = pp[wide(INNER - 1), :]
    for r in reversed(range(INNER)):
        if r < INNER - 1:
            p = pp[wide(r), :] + gg[wide(r), :] * p
        part[wide(r), :] = p
        a = above[wide(r), :]
        b = below[wide(r), :]
        d = p - tgt_l[line(r), :]
        sum_p = sum_p + p
        sum_dd = sum_dd + d * d
        sum_da = sum_da + d * a
        sum_db = sum_db + d * b
    send(2, [p, tip, sum_p, sum_dd])
    send(3, [sum_da, sum_db, sum_bb + 1.0, zero])


def reduced_kernel(got, back):
    groups = [got[pl.ds(g, BLOCKS, stride=4), :].T for g in range(4)]
    q = [groups[i // 4][(i % 4) * TILES:(i % 4 + 1) * TILES] for i in range(15)]
    (a0, b0, u, v, sum_a, sum_b, sum_aa, sum_ab, p0, w, sum_p, sum_dd, sum_da, sum_db, sum_bb) = q
    lane = lax.broadcasted_iota(jnp.int32, (TILES, LANES), 1)
    u = jnp.where(lane == 0, 0.0, u)
    v = jnp.where(lane == BLOCKS - 1, 0.0, v)

    def low(x, s):
        return pltpu.roll(x, s, 1)

    def high(x, s):
        return pltpu.roll(x, LANES - s, 1)

    r = 1.0 / (1.0 - v * high(a0, 1))
    e = u * r
    f = v * high(b0, 1) * r
    d = (w + v * high(p0, 1)) * r
    s = 1
    while s < BLOCKS:
        r = 1.0 / (1.0 - e * low(f, s) - f * high(e, s))
        d = (d + e * low(d, s) + f * high(d, s)) * r
        if 2 * s < BLOCKS:
            e, f = e * low(e, s) * r, f * high(f, s) * r
        s *= 2
    z = d
    x = jnp.where(lane == 0, 0.0, low(z, 1))
    mass = sum_p + sum_a * x + sum_b * z
    error = (
        sum_dd
        + 2.0 * (sum_da * x + sum_db * z + sum_ab * x * z)
        + sum_aa * x * x
        + sum_bb * z * z
    )

    def total(y):
        y = jnp.sum(jnp.sum(y, axis=0, keepdims=True), axis=1, keepdims=True)
        return jnp.broadcast_to(y, (SUB, LANES))

    rest = jnp.zeros((LANES - 2 * TILES - 2 * SUB, LANES), F32)
    back[...] = jnp.concatenate([z, x, total(mass), total(error), rest], axis=0).T


def final_kernel(got, part, above, below, update, totals, lines):
    t = got[...].T
    z = t[:TILES]
    x = t[TILES:2 * TILES]
    scale = 1.0 / (BLOCKS * ROWS * NY)
    totals[0] = jnp.sum(t[2 * TILES:2 * TILES + 1]) * scale
    totals[1] = jnp.sum(t[2 * TILES + SUB:2 * TILES + SUB + 1]) * scale
    for r in range(INNER):
        lines[line(r), :] = part[wide(r), :] + above[wide(r), :] * x + below[wide(r), :] * z
    lines[line(INNER), :] = z
    for h in range(HALVES):
        for i in range(TILES):
            update[h * SUB:(h + 1) * SUB, i * LANES:(i + 1) * LANES] = lines[tile(h, i), :]


def body(history, source, diffusivity, target):
    anywhere = pl.BlockSpec(memory_space=pltpu.HBM)
    vmem = pl.BlockSpec(memory_space=pltpu.VMEM)
    shape = jax.ShapeDtypeStruct
    block = pltpu.VMEM((ROWS, NY), F32)
    tiles = pltpu.VMEM((VREGS * SUB, LANES), F32)
    pair = pltpu.VMEM((2, VREGS * SUB, LANES), F32)
    stages = pltpu.VMEM((STEPS, VREGS * SUB, LANES), F32)
    lines = INNER * TILES
    params = pltpu.CompilerParams(vmem_limit_bytes=48 * 1024 * 1024)
    msg, part, above, below = pl.pallas_call(
        local_kernel,
        name="local",
        out_shape=[shape((4 * BLOCKS, LANES), F32)] + [shape((lines, LANES), F32)] * 3,
        in_specs=[anywhere] * 4,
        out_specs=[vmem] * 4,
        scratch_shapes=[
            pltpu.VMEM((LEVELS, ROWS, NY), F32), block, block, block,
            stages, stages, stages, tiles, pair,
            tiles, tiles, tiles, tiles, tiles, tiles, tiles,
            pltpu.SemaphoreType.DMA((3 + HALVES * CHUNKS,)),
        ],
        compiler_params=params,
    )(*(pltpu.with_memory_space_constraint(x, pltpu.HBM) for x in (history, source, diffusivity, target)))
    got = lax.all_to_all(
        msg.reshape(BLOCKS, 4, LANES), AXIS, split_axis=0, concat_axis=0, tiled=True
    ).reshape(4 * BLOCKS, LANES)
    back = pl.pallas_call(
        reduced_kernel,
        name="reduced",
        out_shape=shape((BLOCKS, LANES), F32),
        in_specs=[vmem],
        out_specs=vmem,
        compiler_params=params,
    )(got)
    solved = lax.all_to_all(back, AXIS, split_axis=0, concat_axis=0, tiled=True)
    return pl.pallas_call(
        final_kernel,
        name="final",
        out_shape=[shape((ROWS, NY), F32), shape((2,), F32)],
        in_specs=[vmem] * 4,
        out_specs=[vmem, pl.BlockSpec(memory_space=pltpu.SMEM)],
        scratch_shapes=[tiles],
        compiler_params=params,
    )(solved, part, above, below)


def solution(mesh):
    return jax.shard_map(
        body,
        mesh=mesh,
        in_specs=(P(None, AXIS, None), P(AXIS, None), P(AXIS, None), P(AXIS, None)),
        out_specs=(P(AXIS, None), P()),
        check_vma=False,
    )
```

```python
import jax
import jax.numpy as jnp
import numpy as np
from jax import lax
from jax.experimental import pallas as pl
from jax.experimental.pallas import tpu as pltpu
from jax.sharding import PartitionSpec as P

STIFF = 1024.0
ORDER = 0.6
AXIS = "rows"
LANES = 128
SUB = 8
LEVELS = 32
ROWS = 16
NY = 4096
TILES = NY // LANES
HALVES = ROWS // SUB
VREGS = HALVES * TILES
BLOCKS = 128
INNER = ROWS - 1
CHUNKS = 4
CHUNK_TILES = TILES // CHUNKS
STEPS = 7
MID = TILES // 2
F32 = jnp.float32


def history_weights():
    moments = np.arange(LEVELS + 1, dtype=np.float64) ** (1.0 - ORDER)
    b = moments[1:] - moments[:-1]
    w = np.concatenate([b[1:], [0.0]]) - np.concatenate([[0.0], b[1:]])
    scale = -w
    scale[0] = 1.0 - w[0]
    return [float(v) for v in scale.astype(np.float32)]


def tile(h, t):
    return pl.ds((h * TILES + t % TILES) * SUB, SUB)


def line(r):
    return pl.ds((r // SUB) * TILES * SUB + r % SUB, TILES, stride=SUB)


def wide(r):
    return pl.ds(r * TILES, TILES)


def lows(load, stride, lane):
    before = pltpu.roll(load(TILES - 1), stride, 1)
    for t in range(TILES):
        down = pltpu.roll(load(t), stride, 1)
        yield jnp.where(lane < stride, before, down)
        before = down


def highs(load, stride, lane):
    back = LANES - stride
    first = here = pltpu.roll(load(0), back, 1)
    for t in range(TILES):
        after = first if t == TILES - 1 else pltpu.roll(load(t + 1), back, 1)
        yield jnp.where(lane >= back, after, here)
        here = after


def local_kernel(
    hist_hbm, src_hbm, dif_hbm, tgt_hbm,
    msg, part, above, below,
    hist, src, dif, tgt,
    couple, inv, main, upper, first, centre, rhs,
    dif_l, tgt_l, sw_l, gg, hh, rr, pp,
    sems,
):
    copies = [
        pltpu.make_async_copy(dif_hbm, dif, sems.at[0]),
        pltpu.make_async_copy(src_hbm, src, sems.at[1]),
    ]
    late = pltpu.make_async_copy(tgt_hbm, tgt, sems.at[HALVES * CHUNKS + 2])
    width = CHUNK_TILES * LANES
    for h in range(HALVES):
        rows = pl.ds(h * SUB, SUB)
        for c in range(CHUNKS):
            cols = pl.ds(c * width, width)
            copies.append(
                pltpu.make_async_copy(
                    hist_hbm.at[:, rows, cols], hist.at[:, rows, cols], sems.at[len(copies)]
                )
            )
    for i, copy in enumerate(copies):
        copy.start()
        if i == CHUNKS + 1:
            late.start()
    lane = lax.broadcasted_iota(jnp.int32, (SUB, LANES), 1)

    copies[0].wait()
    for h in range(HALVES):
        for t in range(TILES):
            c = STIFF * dif[h * SUB:(h + 1) * SUB, t * LANES:(t + 1) * LANES]
            dif_l[tile(h, t), :] = c
            q = 1.0 / c
            first[tile(h, t), :] = q
            m = 2.0 + q
            main[0, tile(h, t), :] = m
            inv[0, tile(h, t), :] = 1.0 / m

    g = h_ = None
    for r in range(ROWS):
        c = dif_l[line(r), :]
        if r == 0:
            q = 1.0 / (1.0 + 2.0 * c)
            g = c * q
            h_ = g
        else:
            q = 1.0 / (1.0 + 2.0 * c - c * g)
            g = c * q
            h_ = g * h_
        rr[wide(r), :] = q
        gg[wide(r), :] = g
        hh[wide(r), :] = h_
    a = hh[wide(INNER - 1), :]
    b = gg[wide(INNER - 1), :]
    zero = jnp.zeros((TILES, LANES), F32)
    sum_a = sum_b = sum_aa = sum_ab = sum_bb = zero
    for r in reversed(range(INNER)):
        if r < INNER - 1:
            g = gg[wide(r), :]
            a = hh[wide(r), :] + g * a
            b = g * b
        above[wide(r), :] = a
        below[wide(r), :] = b
        sum_a = sum_a + a
        sum_b = sum_b + b
        sum_aa = sum_aa + a * a
        sum_ab = sum_ab + a * b
        sum_bb = sum_bb + b * b
    def send(group, four):
        stacked = jnp.concatenate(four, axis=0)
        msg[pl.ds(group, BLOCKS, stride=4), :] = stacked.T

    send(0, [a, b, hh[wide(INNER), :], gg[wide(INNER), :]])
    send(1, [sum_a, sum_b + 1.0, sum_aa, sum_ab])

    for k in range(STEPS):
        stride = 1 << k
        now = k % 2
        for h in range(HALVES):
            def v_of(t):
                return inv[k, tile(h, t), :]

            def p_of(t):
                return v_of(t) if k == 0 else couple[k, tile(h, t), :] * v_of(t)

            def s_of(t):
                return v_of(t) if k == 0 else couple[k, tile(h, t), :] * p_of(t)

            low_v = lows(v_of, stride, lane)
            low_p = low_v if k == 0 else lows(p_of, stride, lane)
            high_s = highs(s_of, stride, lane)
            for t in range(TILES):
                v = next(low_v)
                high = next(high_s)
                if k == 0:
                    b = v
                    if t == 0:
                        b = jnp.where(lane < 2, 0.0, v)
                        v = jnp.where(lane < 1, 0.0, v)
                    if t == TILES - 1:
                        high = jnp.where(lane == LANES - 1, 0.0, high)
                else:
                    b = couple[k, tile(h, t), :]
                    v = b * b * v
                    b = b * next(low_p)
                m = main[now, tile(h, t), :] - v - high
                main[1 - now, tile(h, t), :] = m
                couple[k + 1, tile(h, t), :] = b
                if k < STEPS - 1:
                    inv[k + 1, tile(h, t), :] = 1.0 / m
    for h in range(HALVES):
        a = b = 0.0
        below_b = couple[STEPS, tile(h, 0), :]
        ends = [below_b]
        for step in range(MID):
            t = step
            e = ends.pop()
            f = couple[STEPS, tile(h, t + 1), :]
            ends.append(f)
            q = 1.0 / (main[STEPS % 2, tile(h, t), :] - e * b)
            inv[STEPS, tile(h, t), :] = q
            couple[STEPS, tile(h, t), :] = e * q
            b = f * q
            upper[tile(h, t), :] = b
            t = TILES - 1 - step
            e = couple[STEPS, tile(h, t), :]
            f = below_b
            below_b = e
            q = 1.0 / (main[STEPS % 2, tile(h, t), :] - f * a)
            inv[STEPS, tile(h, t), :] = q
            a = e * q
            couple[STEPS, tile(h, t), :] = a
            upper[tile(h, t), :] = f * q
        centre[pl.ds(h * SUB, SUB), :] = 1.0 / (1.0 - b * a)

    scale = history_weights()
    copies[1].wait()
    for h in range(HALVES):
        rows = slice(h * SUB, (h + 1) * SUB)
        if h == HALVES - 1:
            late.wait()
            for i in range(VREGS):
                g = i // TILES
                t = i % TILES
                tgt_l[tile(g, t), :] = tgt[g * SUB:(g + 1) * SUB, t * LANES:(t + 1) * LANES]
        for c in range(CHUNKS):
            copies[2 + h * CHUNKS + c].wait()
            for t in range(c * CHUNK_TILES, (c + 1) * CHUNK_TILES):
                cols = slice(t * LANES, (t + 1) * LANES)
                acc = src[rows, cols]
                for k in range(LEVELS):
                    acc = acc + scale[k] * hist[k, rows, cols]
                rhs[0, tile(h, t), :] = acc * first[tile(h, t), :]
        for k in range(STEPS):
            now = k % 2

            def z_of(t):
                return inv[k, tile(h, t), :] * rhs[now, tile(h, t), :]

            def y_of(t):
                return z_of(t) if k == 0 else couple[k, tile(h, t), :] * z_of(t)

            low_z = lows(z_of, 1 << k, lane)
            high_y = highs(y_of, 1 << k, lane)
            for t in range(TILES):
                low = next(low_z)
                high = next(high_y)
                if k:
                    low = couple[k, tile(h, t), :] * low
                elif t == 0:
                    low = jnp.where(lane == 0, 0.0, low)
                elif t == TILES - 1:
                    high = jnp.where(lane == LANES - 1, 0.0, high)
                rhs[1 - now, tile(h, t), :] = rhs[now, tile(h, t), :] + low + high
        d = [inv[STEPS, tile(h, t), :] * rhs[STEPS % 2, tile(h, t), :] for t in range(TILES)]
        for step in range(1, MID):
            t = step
            d[t] = d[t] + couple[STEPS, tile(h, t), :] * d[t - 1]
            t = TILES - 1 - step
            d[t] = d[t] + upper[tile(h, t), :] * d[t + 1]
        x = d[MID - 1] + upper[tile(h, MID - 1), :] * d[MID]
        x = x * centre[pl.ds(h * SUB, SUB), :]
        y = d[MID] + couple[STEPS, tile(h, MID), :] * x
        sw_l[tile(h, MID - 1), :] = x
        sw_l[tile(h, MID), :] = y
        for step in range(1, MID):
            t = MID - 1 - step
            x = d[t] + upper[tile(h, t), :] * x
            sw_l[tile(h, t), :] = x
            t = MID + step
            y = d[t] + couple[STEPS, tile(h, t), :] * y
            sw_l[tile(h, t), :] = y

    p = None
    for r in range(ROWS):
        s = rr[wide(r), :] * sw_l[line(r), :]
        p = s if r == 0 else s + gg[wide(r), :] * p
        pp[wide(r), :] = p
    tip = p
    d = tgt_l[line(INNER), :]
    sum_dd = d * d
    sum_db = -d
    sum_da = zero
    sum_p = zero
    p = pp[wide(INNER - 1), :]
    for r in reversed(range(INNER)):
        if r < INNER - 1:
            p = pp[wide(r), :] + gg[wide(r), :] * p
        part[wide(r), :] = p
        a = above[wide(r), :]
        b = below[wide(r), :]
        d = p - tgt_l[line(r), :]
        sum_p = sum_p + p
        sum_dd = sum_dd + d * d
        sum_da = sum_da + d * a
        sum_db = sum_db + d * b
    send(2, [p, tip, sum_p, sum_dd])
    send(3, [sum_da, sum_db, sum_bb + 1.0, zero])


def reduced_kernel(got, back):
    groups = [got[pl.ds(g, BLOCKS, stride=4), :].T for g in range(4)]
    q = [groups[i // 4][(i % 4) * TILES:(i % 4 + 1) * TILES] for i in range(15)]
    (a0, b0, u, v, sum_a, sum_b, sum_aa, sum_ab, p0, w, sum_p, sum_dd, sum_da, sum_db, sum_bb) = q
    lane = lax.broadcasted_iota(jnp.int32, (TILES, LANES), 1)
    u = jnp.where(lane == 0, 0.0, u)
    v = jnp.where(lane == BLOCKS - 1, 0.0, v)

    def low(x, s):
        return pltpu.roll(x, s, 1)

    def high(x, s):
        return pltpu.roll(x, LANES - s, 1)

    r = 1.0 / (1.0 - v * high(a0, 1))
    e = u * r
    f = v * high(b0, 1) * r
    d = (w + v * high(p0, 1)) * r
    s = 1
    while s < BLOCKS:
        r = 1.0 / (1.0 - e * low(f, s) - f * high(e, s))
        d = (d + e * low(d, s) + f * high(d, s)) * r
        if 2 * s < BLOCKS:
            e, f = e * low(e, s) * r, f * high(f, s) * r
        s *= 2
    z = d
    x = jnp.where(lane == 0, 0.0, low(z, 1))
    mass = sum_p + sum_a * x + sum_b * z
    error = (
        sum_dd
        + 2.0 * (sum_da * x + sum_db * z + sum_ab * x * z)
        + sum_aa * x * x
        + sum_bb * z * z
    )

    def total(y):
        y = jnp.sum(jnp.sum(y, axis=0, keepdims=True), axis=1, keepdims=True)
        return jnp.broadcast_to(y, (SUB, LANES))

    rest = jnp.zeros((LANES - 2 * TILES - 2 * SUB, LANES), F32)
    back[...] = jnp.concatenate([z, x, total(mass), total(error), rest], axis=0).T


def final_kernel(got, part, above, below, update, totals, lines):
    t = got[...].T
    z = t[:TILES]
    x = t[TILES:2 * TILES]
    scale = 1.0 / (BLOCKS * ROWS * NY)
    totals[0] = jnp.sum(t[2 * TILES:2 * TILES + 1]) * scale
    totals[1] = jnp.sum(t[2 * TILES + SUB:2 * TILES + SUB + 1]) * scale
    for r in range(INNER):
        lines[line(r), :] = part[wide(r), :] + above[wide(r), :] * x + below[wide(r), :] * z
    lines[line(INNER), :] = z
    for h in range(HALVES):
        for i in range(TILES):
            update[h * SUB:(h + 1) * SUB, i * LANES:(i + 1) * LANES] = lines[tile(h, i), :]


def body(history, source, diffusivity, target):
    anywhere = pl.BlockSpec(memory_space=pltpu.HBM)
    vmem = pl.BlockSpec(memory_space=pltpu.VMEM)
    shape = jax.ShapeDtypeStruct
    block = pltpu.VMEM((ROWS, NY), F32)
    tiles = pltpu.VMEM((VREGS * SUB, LANES), F32)
    pair = pltpu.VMEM((2, VREGS * SUB, LANES), F32)
    stages = pltpu.VMEM((STEPS + 1, VREGS * SUB, LANES), F32)
    block_tile = pltpu.VMEM((ROWS, LANES), F32)
    lines = INNER * TILES
    params = pltpu.CompilerParams(vmem_limit_bytes=48 * 1024 * 1024)
    msg, part, above, below = pl.pallas_call(
        local_kernel,
        name="local",
        out_shape=[shape((4 * BLOCKS, LANES), F32)] + [shape((lines, LANES), F32)] * 3,
        in_specs=[anywhere] * 4,
        out_specs=[vmem] * 4,
        scratch_shapes=[
            pltpu.VMEM((LEVELS, ROWS, NY), F32), block, block, block,
            stages, stages, pair, tiles, tiles, block_tile, pair,
            tiles, tiles, tiles, tiles, tiles, tiles, tiles,
            pltpu.SemaphoreType.DMA((3 + HALVES * CHUNKS,)),
        ],
        compiler_params=params,
    )(*(pltpu.with_memory_space_constraint(x, pltpu.HBM) for x in (history, source, diffusivity, target)))
    got = lax.all_to_all(
        msg.reshape(BLOCKS, 4, LANES), AXIS, split_axis=0, concat_axis=0, tiled=True
    ).reshape(4 * BLOCKS, LANES)
    back = pl.pallas_call(
        reduced_kernel,
        name="reduced",
        out_shape=shape((BLOCKS, LANES), F32),
        in_specs=[vmem],
        out_specs=vmem,
        compiler_params=params,
    )(got)
    solved = lax.all_to_all(back, AXIS, split_axis=0, concat_axis=0, tiled=True)
    return pl.pallas_call(
        final_kernel,
        name="final",
        out_shape=[shape((ROWS, NY), F32), shape((2,), F32)],
        in_specs=[vmem] * 4,
        out_specs=[vmem, pl.BlockSpec(memory_space=pltpu.SMEM)],
        scratch_shapes=[tiles],
        compiler_params=params,
    )(solved, part, above, below)


def solution(mesh):
    return jax.shard_map(
        body,
        mesh=mesh,
        in_specs=(P(None, AXIS, None), P(AXIS, None), P(AXIS, None), P(AXIS, None)),
        out_specs=(P(AXIS, None), P()),
        check_vma=False,
    )
```

```python
import jax
import jax.numpy as jnp
import numpy as np
from jax import lax
from jax.experimental import pallas as pl
from jax.experimental.pallas import tpu as pltpu
from jax.sharding import PartitionSpec as P

STIFF = 1024.0
ORDER = 0.6
AXIS = "rows"
LANES = 128
SUB = 8
LEVELS = 32
ROWS = 16
NY = 4096
TILES = NY // LANES
HALVES = ROWS // SUB
VREGS = HALVES * TILES
BLOCKS = 128
INNER = ROWS - 1
CHUNKS = 4
CHUNK_TILES = TILES // CHUNKS
STEPS = 7
MID = TILES // 2
F32 = jnp.float32


def history_weights():
    moments = np.arange(LEVELS + 1, dtype=np.float64) ** (1.0 - ORDER)
    b = moments[1:] - moments[:-1]
    w = np.concatenate([b[1:], [0.0]]) - np.concatenate([[0.0], b[1:]])
    scale = -w
    scale[0] = 1.0 - w[0]
    return [float(v) for v in scale.astype(np.float32)]


def tile(h, t):
    return pl.ds((h * TILES + t % TILES) * SUB, SUB)


def line(r):
    return pl.ds((r // SUB) * TILES * SUB + r % SUB, TILES, stride=SUB)


def wide(r):
    return pl.ds(r * TILES, TILES)


def lows(load, stride, lane):
    before = pltpu.roll(load(TILES - 1), stride, 1)
    for t in range(TILES):
        down = pltpu.roll(load(t), stride, 1)
        yield jnp.where(lane < stride, before, down)
        before = down


def highs(load, stride, lane):
    back = LANES - stride
    first = here = pltpu.roll(load(0), back, 1)
    for t in range(TILES):
        after = first if t == TILES - 1 else pltpu.roll(load(t + 1), back, 1)
        yield jnp.where(lane >= back, after, here)
        here = after


def both(load, lane):
    half = LANES // 2
    last = before = pltpu.roll(load(TILES - 1), half, 1)
    first = here = pltpu.roll(load(0), half, 1)
    for t in range(TILES):
        if t == TILES - 1:
            after = first
        elif t == TILES - 2:
            after = last
        else:
            after = pltpu.roll(load(t + 1), half, 1)
        yield jnp.where(lane < half, before, here), jnp.where(lane >= half, after, here)
        before, here = here, after


def local_kernel(
    hist_hbm, src_hbm, dif_hbm, tgt_hbm,
    msg, part, above, below,
    hist, src, dif, tgt,
    couple, inv, main, upper, beyond, first, centre, rhs,
    dif_l, tgt_l, sw_l, gg, hh, rr, pp,
    weights, sems,
):
    copies = [
        pltpu.make_async_copy(dif_hbm, dif, sems.at[0]),
        pltpu.make_async_copy(src_hbm, src, sems.at[1]),
    ]
    late = pltpu.make_async_copy(tgt_hbm, tgt, sems.at[HALVES * CHUNKS + 2])
    width = CHUNK_TILES * LANES
    for h in range(HALVES):
        rows = pl.ds(h * SUB, SUB)
        for c in range(CHUNKS):
            cols = pl.ds(c * width, width)
            copies.append(
                pltpu.make_async_copy(
                    hist_hbm.at[:, rows, cols], hist.at[:, rows, cols], sems.at[len(copies)]
                )
            )
    for i, copy in enumerate(copies):
        copy.start()
        if i == CHUNKS + 1:
            late.start()
    lane = lax.broadcasted_iota(jnp.int32, (SUB, LANES), 1)
    for k, value in enumerate(history_weights()):
        weights[pl.ds(k * SUB, SUB), :] = jnp.full((SUB, LANES), value, F32)

    copies[0].wait()
    for h in range(HALVES):
        for t in range(TILES):
            c = STIFF * dif[h * SUB:(h + 1) * SUB, t * LANES:(t + 1) * LANES]
            dif_l[tile(h, t), :] = c
            q = 1.0 / c
            first[tile(h, t), :] = q
            u = 0.5 * q * (1.0 / (2.0 + q))
            couple[0, tile(h, t), :] = u
            inv[0, tile(h, t), :] = 0.5 - u

    g = h_ = None
    for r in range(ROWS):
        c = dif_l[line(r), :]
        if r == 0:
            q = 1.0 / (1.0 + 2.0 * c)
            g = c * q
            h_ = g
        else:
            q = 1.0 / (1.0 + 2.0 * c - c * g)
            g = c * q
            h_ = g * h_
        rr[wide(r), :] = q
        gg[wide(r), :] = g
        hh[wide(r), :] = h_
    a = hh[wide(INNER - 1), :]
    b = gg[wide(INNER - 1), :]
    zero = jnp.zeros((TILES, LANES), F32)
    sum_a = sum_b = sum_aa = sum_ab = sum_bb = zero
    for r in reversed(range(INNER)):
        if r < INNER - 1:
            g = gg[wide(r), :]
            a = hh[wide(r), :] + g * a
            b = g * b
        above[wide(r), :] = a
        below[wide(r), :] = b
        sum_a = sum_a + a
        sum_b = sum_b + b
        sum_aa = sum_aa + a * a
        sum_ab = sum_ab + a * b
        sum_bb = sum_bb + b * b
    def send(group, four):
        stacked = jnp.concatenate(four, axis=0)
        msg[pl.ds(group, BLOCKS, stride=4), :] = stacked.T

    send(0, [a, b, hh[wide(INNER), :], gg[wide(INNER), :]])
    send(1, [sum_a, sum_b + 1.0, sum_aa, sum_ab])

    def bands(h):
        low_u = lows(lambda t: couple[0, tile(h, t), :], 1, lane)
        high_u = highs(lambda t: couple[0, tile(h, t), :], 1, lane)
        for t in range(TILES):
            low = next(low_u)
            high = next(high_u)
            q = first[tile(h, t), :]
            m = 1.0 + (q + low + high)
            b = 0.5 - low
            if t == 0:
                m = jnp.where(lane == 0, 1.5 + (q + high), m)
                b = jnp.where(lane < 2, 0.0, b)
            if t == TILES - 1:
                m = jnp.where(lane == LANES - 1, 1.5 + (q + low), m)
            main[1, tile(h, t), :] = m
            couple[1, tile(h, t), :] = b
            inv[1, tile(h, t), :] = 1.0 / m
            yield
        for k in range(1, STEPS):
            stride = 1 << k
            now = k % 2

            def v_of(t):
                return inv[k, tile(h, t), :]

            def p_of(t):
                return couple[k, tile(h, t), :] * v_of(t)

            if k == STEPS - 1:
                pairs_v = both(v_of, lane)
                pairs_b = both(lambda t: couple[k, tile(h, t), :], lane)
                for t in range(TILES):
                    b = couple[k, tile(h, t), :]
                    low_v, high_v = next(pairs_v)
                    low_b, high_b = next(pairs_b)
                    beyond[tile(h, t), :] = high_b
                    m = main[now, tile(h, t), :] - b * b * low_v - high_b * high_b * high_v
                    main[1 - now, tile(h, t), :] = m
                    couple[k + 1, tile(h, t), :] = b * low_b * low_v
                    yield
                continue
            low_v = lows(v_of, stride, lane)
            low_p = lows(p_of, stride, lane)
            high_s = highs(lambda t: couple[k, tile(h, t), :] * p_of(t), stride, lane)
            for t in range(TILES):
                b = couple[k, tile(h, t), :]
                m = main[now, tile(h, t), :] - b * b * next(low_v) - next(high_s)
                main[1 - now, tile(h, t), :] = m
                couple[k + 1, tile(h, t), :] = b * next(low_p)
                inv[k + 1, tile(h, t), :] = 1.0 / m
                yield
        a = b = 0.0
        below_b = couple[STEPS, tile(h, 0), :]
        ends = [below_b]
        for step in range(MID):
            t = step
            e = ends.pop()
            f = couple[STEPS, tile(h, t + 1), :]
            ends.append(f)
            q = 1.0 / (main[STEPS % 2, tile(h, t), :] - e * b)
            inv[STEPS, tile(h, t), :] = q
            couple[STEPS, tile(h, t), :] = e * q
            b = f * q
            upper[tile(h, t), :] = b
            t = TILES - 1 - step
            e = couple[STEPS, tile(h, t), :]
            f = below_b
            below_b = e
            q = 1.0 / (main[STEPS % 2, tile(h, t), :] - f * a)
            inv[STEPS, tile(h, t), :] = q
            a = e * q
            couple[STEPS, tile(h, t), :] = a
            upper[tile(h, t), :] = f * q
            yield
        centre[pl.ds(h * SUB, SUB), :] = 1.0 / (1.0 - b * a)

    def drive(h, c):
        rows = slice(h * SUB, (h + 1) * SUB)
        own = range(c * CHUNK_TILES, (c + 1) * CHUNK_TILES)
        acc = [src[rows, t * LANES:(t + 1) * LANES] for t in own]
        for k in range(LEVELS):
            weight = weights[pl.ds(k * SUB, SUB), :]
            for i, t in enumerate(own):
                acc[i] = acc[i] + weight * hist[k, rows, t * LANES:(t + 1) * LANES]
        for i, t in enumerate(own):
            rhs[0, tile(h, t), :] = acc[i] * first[tile(h, t), :]

    def right_side(h):
        for k in range(STEPS):
            now = k % 2

            def z_of(t):
                return inv[k, tile(h, t), :] * rhs[now, tile(h, t), :]

            def y_of(t):
                return z_of(t) if k == 0 else couple[k, tile(h, t), :] * z_of(t)

            if k == STEPS - 1:
                pairs_z = both(z_of, lane)
                for t in range(TILES):
                    low, high = next(pairs_z)
                    low = couple[k, tile(h, t), :] * low
                    high = beyond[tile(h, t), :] * high
                    rhs[1 - now, tile(h, t), :] = rhs[now, tile(h, t), :] + low + high
                continue
            low_z = lows(z_of, 1 << k, lane)
            high_y = highs(y_of, 1 << k, lane)
            for t in range(TILES):
                low = next(low_z)
                high = next(high_y)
                if k:
                    low = couple[k, tile(h, t), :] * low
                elif t == 0:
                    low = jnp.where(lane == 0, 0.0, low)
                elif t == TILES - 1:
                    high = jnp.where(lane == LANES - 1, 0.0, high)
                rhs[1 - now, tile(h, t), :] = rhs[now, tile(h, t), :] + low + high
        d = [inv[STEPS, tile(h, t), :] * rhs[STEPS % 2, tile(h, t), :] for t in range(TILES)]
        for step in range(1, MID):
            t = step
            d[t] = d[t] + couple[STEPS, tile(h, t), :] * d[t - 1]
            t = TILES - 1 - step
            d[t] = d[t] + upper[tile(h, t), :] * d[t + 1]
        x = d[MID - 1] + upper[tile(h, MID - 1), :] * d[MID]
        x = x * centre[pl.ds(h * SUB, SUB), :]
        y = d[MID] + couple[STEPS, tile(h, MID), :] * x
        sw_l[tile(h, MID - 1), :] = x
        sw_l[tile(h, MID), :] = y
        for step in range(1, MID):
            t = MID - 1 - step
            x = d[t] + upper[tile(h, t), :] * x
            sw_l[tile(h, t), :] = x
            t = MID + step
            y = d[t] + couple[STEPS, tile(h, t), :] * y
            sw_l[tile(h, t), :] = y

    halves = [bands(h) for h in range(HALVES)]
    for k in range(STEPS + 1):
        for half in halves:
            for _ in range(TILES):
                next(half, None)

    copies[1].wait()
    for h in range(HALVES):
        if h == HALVES - 1:
            late.wait()
            for i in range(VREGS):
                g = i // TILES
                t = i % TILES
                tgt_l[tile(g, t), :] = tgt[g * SUB:(g + 1) * SUB, t * LANES:(t + 1) * LANES]
        for c in range(CHUNKS):
            copies[2 + h * CHUNKS + c].wait()
            drive(h, c)
        right_side(h)

    p = None
    for r in range(ROWS):
        s = rr[wide(r), :] * sw_l[line(r), :]
        p = s if r == 0 else s + gg[wide(r), :] * p
        pp[wide(r), :] = p
    tip = p
    d = tgt_l[line(INNER), :]
    sum_dd = d * d
    sum_db = -d
    sum_da = zero
    sum_p = zero
    p = pp[wide(INNER - 1), :]
    for r in reversed(range(INNER)):
        if r < INNER - 1:
            p = pp[wide(r), :] + gg[wide(r), :] * p
        part[wide(r), :] = p
        a = above[wide(r), :]
        b = below[wide(r), :]
        d = p - tgt_l[line(r), :]
        sum_p = sum_p + p
        sum_dd = sum_dd + d * d
        sum_da = sum_da + d * a
        sum_db = sum_db + d * b
    send(2, [p, tip, sum_p, sum_dd])
    send(3, [sum_da, sum_db, sum_bb + 1.0, zero])


def reduced_kernel(got, back):
    groups = [got[pl.ds(g, BLOCKS, stride=4), :].T for g in range(4)]
    q = [groups[i // 4][(i % 4) * TILES:(i % 4 + 1) * TILES] for i in range(15)]
    (a0, b0, u, v, sum_a, sum_b, sum_aa, sum_ab, p0, w, sum_p, sum_dd, sum_da, sum_db, sum_bb) = q
    lane = lax.broadcasted_iota(jnp.int32, (TILES, LANES), 1)
    u = jnp.where(lane == 0, 0.0, u)
    v = jnp.where(lane == BLOCKS - 1, 0.0, v)

    def low(x, s):
        return pltpu.roll(x, s, 1)

    def high(x, s):
        return pltpu.roll(x, LANES - s, 1)

    r = 1.0 / (1.0 - v * high(a0, 1))
    e = u * r
    f = v * high(b0, 1) * r
    d = (w + v * high(p0, 1)) * r
    s = 1
    while s < BLOCKS:
        r = 1.0 / (1.0 - e * low(f, s) - f * high(e, s))
        d = (d + e * low(d, s) + f * high(d, s)) * r
        if 2 * s < BLOCKS:
            e, f = e * low(e, s) * r, f * high(f, s) * r
        s *= 2
    z = d
    x = jnp.where(lane == 0, 0.0, low(z, 1))
    mass = sum_p + sum_a * x + sum_b * z
    error = (
        sum_dd
        + 2.0 * (sum_da * x + sum_db * z + sum_ab * x * z)
        + sum_aa * x * x
        + sum_bb * z * z
    )

    def total(y):
        y = jnp.sum(jnp.sum(y, axis=0, keepdims=True), axis=1, keepdims=True)
        return jnp.broadcast_to(y, (SUB, LANES))

    rest = jnp.zeros((LANES - 2 * TILES - 2 * SUB, LANES), F32)
    back[...] = jnp.concatenate([z, x, total(mass), total(error), rest], axis=0).T


def final_kernel(got, part, above, below, update, totals, lines):
    t = got[...].T
    z = t[:TILES]
    x = t[TILES:2 * TILES]
    scale = 1.0 / (BLOCKS * ROWS * NY)
    totals[0] = jnp.sum(t[2 * TILES:2 * TILES + 1]) * scale
    totals[1] = jnp.sum(t[2 * TILES + SUB:2 * TILES + SUB + 1]) * scale
    for r in range(INNER):
        lines[line(r), :] = part[wide(r), :] + above[wide(r), :] * x + below[wide(r), :] * z
    lines[line(INNER), :] = z
    for h in range(HALVES):
        for i in range(TILES):
            update[h * SUB:(h + 1) * SUB, i * LANES:(i + 1) * LANES] = lines[tile(h, i), :]


def body(history, source, diffusivity, target):
    anywhere = pl.BlockSpec(memory_space=pltpu.HBM)
    vmem = pl.BlockSpec(memory_space=pltpu.VMEM)
    shape = jax.ShapeDtypeStruct
    block = pltpu.VMEM((ROWS, NY), F32)
    tiles = pltpu.VMEM((VREGS * SUB, LANES), F32)
    pair = pltpu.VMEM((2, VREGS * SUB, LANES), F32)
    stages = pltpu.VMEM((STEPS + 1, VREGS * SUB, LANES), F32)
    block_tile = pltpu.VMEM((ROWS, LANES), F32)
    lines = INNER * TILES
    params = pltpu.CompilerParams(vmem_limit_bytes=48 * 1024 * 1024)
    msg, part, above, below = pl.pallas_call(
        local_kernel,
        name="local",
        out_shape=[shape((4 * BLOCKS, LANES), F32)] + [shape((lines, LANES), F32)] * 3,
        in_specs=[anywhere] * 4,
        out_specs=[vmem] * 4,
        scratch_shapes=[
            pltpu.VMEM((LEVELS, ROWS, NY), F32), block, block, block,
            stages, stages, pair, tiles, tiles, tiles, block_tile, pair,
            tiles, tiles, tiles, tiles, tiles, tiles, tiles,
            pltpu.VMEM((LEVELS * SUB, LANES), F32),
            pltpu.SemaphoreType.DMA((3 + HALVES * CHUNKS,)),
        ],
        compiler_params=params,
    )(*(pltpu.with_memory_space_constraint(x, pltpu.HBM) for x in (history, source, diffusivity, target)))
    got = lax.all_to_all(
        msg.reshape(BLOCKS, 4, LANES), AXIS, split_axis=0, concat_axis=0, tiled=True
    ).reshape(4 * BLOCKS, LANES)
    back = pl.pallas_call(
        reduced_kernel,
        name="reduced",
        out_shape=shape((BLOCKS, LANES), F32),
        in_specs=[vmem],
        out_specs=vmem,
        compiler_params=params,
    )(got)
    solved = lax.all_to_all(back, AXIS, split_axis=0, concat_axis=0, tiled=True)
    return pl.pallas_call(
        final_kernel,
        name="final",
        out_shape=[shape((ROWS, NY), F32), shape((2,), F32)],
        in_specs=[vmem] * 4,
        out_specs=[vmem, pl.BlockSpec(memory_space=pltpu.SMEM)],
        scratch_shapes=[tiles],
        compiler_params=params,
    )(solved, part, above, below)


def solution(mesh):
    return jax.shard_map(
        body,
        mesh=mesh,
        in_specs=(P(None, AXIS, None), P(AXIS, None), P(AXIS, None), P(AXIS, None)),
        out_specs=(P(AXIS, None), P()),
        check_vma=False,
    )
```

```python
import jax
import jax.numpy as jnp
import numpy as np
from jax import lax
from jax.experimental import pallas as pl
from jax.experimental.pallas import tpu as pltpu
from jax.sharding import PartitionSpec as P

STIFF = 1024.0
ORDER = 0.6
AXIS = "rows"
LANES = 128
SUB = 8
LEVELS = 32
ROWS = 16
NY = 4096
TILES = NY // LANES
HALVES = ROWS // SUB
VREGS = HALVES * TILES
BLOCKS = 128
INNER = ROWS - 1
CHUNKS = 4
CHUNK_TILES = TILES // CHUNKS
STEPS = 7
MID = TILES // 2
F32 = jnp.float32


def history_weights():
    moments = np.arange(LEVELS + 1, dtype=np.float64) ** (1.0 - ORDER)
    b = moments[1:] - moments[:-1]
    w = np.concatenate([b[1:], [0.0]]) - np.concatenate([[0.0], b[1:]])
    scale = -w
    scale[0] = 1.0 - w[0]
    return [float(v) for v in scale.astype(np.float32)]


def tile(h, t):
    return pl.ds((h * TILES + t % TILES) * SUB, SUB)


def line(r):
    return pl.ds((r // SUB) * TILES * SUB + r % SUB, TILES, stride=SUB)


def wide(r):
    return pl.ds(r * TILES, TILES)


def lows(load, stride, lane):
    before = pltpu.roll(load(TILES - 1), stride, 1)
    for t in range(TILES):
        down = pltpu.roll(load(t), stride, 1)
        yield jnp.where(lane < stride, before, down)
        before = down


def highs(load, stride, lane):
    back = LANES - stride
    first = here = pltpu.roll(load(0), back, 1)
    for t in range(TILES):
        after = first if t == TILES - 1 else pltpu.roll(load(t + 1), back, 1)
        yield jnp.where(lane >= back, after, here)
        here = after


def both(load, lane):
    half = LANES // 2
    last = before = pltpu.roll(load(TILES - 1), half, 1)
    first = here = pltpu.roll(load(0), half, 1)
    for t in range(TILES):
        if t == TILES - 1:
            after = first
        elif t == TILES - 2:
            after = last
        else:
            after = pltpu.roll(load(t + 1), half, 1)
        yield jnp.where(lane < half, before, here), jnp.where(lane >= half, after, here)
        before, here = here, after


def local_kernel(
    hist_hbm, src_hbm, dif_hbm, tgt_hbm,
    msg, part, above, below,
    hist, src, dif, tgt,
    couple, inv, main, upper, beyond, first, centre, rhs,
    dif_l, tgt_l, sw_l, gg, hh, rr, pp,
    weights, sems,
):
    copies = [
        pltpu.make_async_copy(dif_hbm, dif, sems.at[0]),
        pltpu.make_async_copy(src_hbm, src, sems.at[1]),
    ]
    late = pltpu.make_async_copy(tgt_hbm, tgt, sems.at[HALVES * CHUNKS + 2])
    width = CHUNK_TILES * LANES
    for h in range(HALVES):
        rows = pl.ds(h * SUB, SUB)
        for c in range(CHUNKS):
            cols = pl.ds(c * width, width)
            copies.append(
                pltpu.make_async_copy(
                    hist_hbm.at[:, rows, cols], hist.at[:, rows, cols], sems.at[len(copies)]
                )
            )
    for i, copy in enumerate(copies):
        copy.start()
        if i == CHUNKS + 1:
            late.start()
    lane = lax.broadcasted_iota(jnp.int32, (SUB, LANES), 1)
    for k, value in enumerate(history_weights()):
        weights[pl.ds(k * SUB, SUB), :] = jnp.full((SUB, LANES), value, F32)

    copies[0].wait()
    for h in range(HALVES):
        for t in range(TILES):
            c = STIFF * dif[h * SUB:(h + 1) * SUB, t * LANES:(t + 1) * LANES]
            dif_l[tile(h, t), :] = c
            q = 1.0 / c
            first[tile(h, t), :] = q
            u = 0.5 * q * (1.0 / (2.0 + q))
            couple[0, tile(h, t), :] = u
            inv[0, tile(h, t), :] = 0.5 - u

    g = h_ = None
    for r in range(ROWS):
        c = dif_l[line(r), :]
        if r == 0:
            q = 1.0 / (1.0 + 2.0 * c)
            g = c * q
            h_ = g
        else:
            q = 1.0 / (1.0 + 2.0 * c - c * g)
            g = c * q
            h_ = g * h_
        rr[wide(r), :] = q
        gg[wide(r), :] = g
        hh[wide(r), :] = h_
    a = hh[wide(INNER - 1), :]
    b = gg[wide(INNER - 1), :]
    zero = jnp.zeros((TILES, LANES), F32)
    sum_a = sum_b = sum_aa = sum_ab = sum_bb = zero
    for r in reversed(range(INNER)):
        if r < INNER - 1:
            g = gg[wide(r), :]
            a = hh[wide(r), :] + g * a
            b = g * b
        above[wide(r), :] = a
        below[wide(r), :] = b
        sum_a = sum_a + a
        sum_b = sum_b + b
        sum_aa = sum_aa + a * a
        sum_ab = sum_ab + a * b
        sum_bb = sum_bb + b * b
    def send(group, four):
        stacked = jnp.concatenate(four, axis=0)
        msg[pl.ds(group, BLOCKS, stride=4), :] = stacked.T

    send(0, [a, b, hh[wide(INNER), :], gg[wide(INNER), :]])
    send(1, [sum_a, sum_b + 1.0, sum_aa, sum_ab])

    def bands(h):
        low_u = lows(lambda t: couple[0, tile(h, t), :], 1, lane)
        high_u = highs(lambda t: couple[0, tile(h, t), :], 1, lane)
        for t in range(TILES):
            low = next(low_u)
            high = next(high_u)
            q = first[tile(h, t), :]
            m = 1.0 + (q + low + high)
            b = 0.5 - low
            if t == 0:
                m = jnp.where(lane == 0, 1.5 + (q + high), m)
                b = jnp.where(lane < 2, 0.0, b)
            if t == TILES - 1:
                m = jnp.where(lane == LANES - 1, 1.5 + (q + low), m)
            main[1, tile(h, t), :] = m
            couple[1, tile(h, t), :] = b
            inv[1, tile(h, t), :] = 1.0 / m
            yield
        for k in range(1, STEPS):
            stride = 1 << k
            now = k % 2

            def v_of(t):
                return inv[k, tile(h, t), :]

            def p_of(t):
                return couple[k, tile(h, t), :] * v_of(t)

            if k == STEPS - 1:
                pairs_v = both(v_of, lane)
                pairs_b = both(lambda t: couple[k, tile(h, t), :], lane)
                for t in range(TILES):
                    b = couple[k, tile(h, t), :]
                    low_v, high_v = next(pairs_v)
                    low_b, high_b = next(pairs_b)
                    beyond[tile(h, t), :] = high_b
                    m = main[now, tile(h, t), :] - b * b * low_v - high_b * high_b * high_v
                    main[1 - now, tile(h, t), :] = m
                    couple[k + 1, tile(h, t), :] = b * low_b * low_v
                    yield
                continue
            low_v = lows(v_of, stride, lane)
            low_p = lows(p_of, stride, lane)
            high_s = highs(lambda t: couple[k, tile(h, t), :] * p_of(t), stride, lane)
            for t in range(TILES):
                b = couple[k, tile(h, t), :]
                m = main[now, tile(h, t), :] - b * b * next(low_v) - next(high_s)
                main[1 - now, tile(h, t), :] = m
                couple[k + 1, tile(h, t), :] = b * next(low_p)
                inv[k + 1, tile(h, t), :] = 1.0 / m
                yield
        a = b = 0.0
        below_b = couple[STEPS, tile(h, 0), :]
        ends = [below_b]
        for step in range(MID):
            t = step
            e = ends.pop()
            f = couple[STEPS, tile(h, t + 1), :]
            ends.append(f)
            q = 1.0 / (main[STEPS % 2, tile(h, t), :] - e * b)
            inv[STEPS, tile(h, t), :] = q
            couple[STEPS, tile(h, t), :] = e * q
            b = f * q
            upper[tile(h, t), :] = b
            t = TILES - 1 - step
            e = couple[STEPS, tile(h, t), :]
            f = below_b
            below_b = e
            q = 1.0 / (main[STEPS % 2, tile(h, t), :] - f * a)
            inv[STEPS, tile(h, t), :] = q
            a = e * q
            couple[STEPS, tile(h, t), :] = a
            upper[tile(h, t), :] = f * q
            yield
        centre[pl.ds(h * SUB, SUB), :] = 1.0 / (1.0 - b * a)

    def drive(h, c):
        rows = slice(h * SUB, (h + 1) * SUB)
        own = range(c * CHUNK_TILES, (c + 1) * CHUNK_TILES)
        acc = [src[rows, t * LANES:(t + 1) * LANES] for t in own]
        for k in range(LEVELS):
            weight = weights[pl.ds(k * SUB, SUB), :]
            for i, t in enumerate(own):
                acc[i] = acc[i] + weight * hist[k, rows, t * LANES:(t + 1) * LANES]
        for i, t in enumerate(own):
            rhs[0, tile(h, t), :] = acc[i] * first[tile(h, t), :]

    def right_side(h):
        for k in range(STEPS):
            now = k % 2

            def z_of(t):
                return inv[k, tile(h, t), :] * rhs[now, tile(h, t), :]

            def y_of(t):
                return z_of(t) if k == 0 else couple[k, tile(h, t), :] * z_of(t)

            if k == STEPS - 1:
                pairs_z = both(z_of, lane)
                for t in range(TILES):
                    low, high = next(pairs_z)
                    low = couple[k, tile(h, t), :] * low
                    high = beyond[tile(h, t), :] * high
                    rhs[1 - now, tile(h, t), :] = rhs[now, tile(h, t), :] + low + high
                continue
            low_z = lows(z_of, 1 << k, lane)
            high_y = highs(y_of, 1 << k, lane)
            for t in range(TILES):
                low = next(low_z)
                high = next(high_y)
                if k:
                    low = couple[k, tile(h, t), :] * low
                elif t == 0:
                    low = jnp.where(lane == 0, 0.0, low)
                elif t == TILES - 1:
                    high = jnp.where(lane == LANES - 1, 0.0, high)
                rhs[1 - now, tile(h, t), :] = rhs[now, tile(h, t), :] + low + high
        d = [inv[STEPS, tile(h, t), :] * rhs[STEPS % 2, tile(h, t), :] for t in range(TILES)]
        for step in range(1, MID):
            t = step
            d[t] = d[t] + couple[STEPS, tile(h, t), :] * d[t - 1]
            t = TILES - 1 - step
            d[t] = d[t] + upper[tile(h, t), :] * d[t + 1]
        x = d[MID - 1] + upper[tile(h, MID - 1), :] * d[MID]
        x = x * centre[pl.ds(h * SUB, SUB), :]
        y = d[MID] + couple[STEPS, tile(h, MID), :] * x
        sw_l[tile(h, MID - 1), :] = x
        sw_l[tile(h, MID), :] = y
        for step in range(1, MID):
            t = MID - 1 - step
            x = d[t] + upper[tile(h, t), :] * x
            sw_l[tile(h, t), :] = x
            t = MID + step
            y = d[t] + couple[STEPS, tile(h, t), :] * y
            sw_l[tile(h, t), :] = y

    halves = [bands(h) for h in range(HALVES)]
    for k in range(STEPS + 1):
        for half in halves:
            for _ in range(TILES):
                next(half, None)

    copies[1].wait()
    for h in range(HALVES):
        if h == HALVES - 1:
            late.wait()
            for i in range(VREGS):
                g = i // TILES
                t = i % TILES
                tgt_l[tile(g, t), :] = tgt[g * SUB:(g + 1) * SUB, t * LANES:(t + 1) * LANES]
        for c in range(CHUNKS):
            copies[2 + h * CHUNKS + c].wait()
            drive(h, c)
        right_side(h)

    p = None
    for r in range(ROWS):
        s = rr[wide(r), :] * sw_l[line(r), :]
        p = s if r == 0 else s + gg[wide(r), :] * p
        pp[wide(r), :] = p
    tip = p
    d = tgt_l[line(INNER), :]
    sum_dd = d * d
    sum_db = -d
    sum_da = zero
    sum_p = zero
    p = pp[wide(INNER - 1), :]
    for r in reversed(range(INNER)):
        if r < INNER - 1:
            p = pp[wide(r), :] + gg[wide(r), :] * p
        part[wide(r), :] = p
        a = above[wide(r), :]
        b = below[wide(r), :]
        d = p - tgt_l[line(r), :]
        sum_p = sum_p + p
        sum_dd = sum_dd + d * d
        sum_da = sum_da + d * a
        sum_db = sum_db + d * b
    send(2, [p, tip, sum_p, sum_dd])
    send(3, [sum_da, sum_db, sum_bb + 1.0, zero])


def reduced_kernel(got, back, left, right, value):
    groups = [got[pl.ds(g, BLOCKS, stride=4), :] for g in range(4)]
    edge = jnp.zeros((SUB, LANES), F32)
    for ref in (left, right, value):
        ref[pl.ds(0, SUB), :] = edge
        ref[pl.ds(SUB + BLOCKS, SUB), :] = edge
    inside = pl.ds(SUB, BLOCKS)

    def low(x, ref, s):
        if s < SUB:
            return ref[pl.ds(SUB - s, BLOCKS), :]
        return jnp.concatenate([jnp.zeros((s, LANES), F32), x[:BLOCKS - s]], axis=0)

    def high(x, ref, s):
        if s < SUB:
            return ref[pl.ds(SUB + s, BLOCKS), :]
        return jnp.concatenate([x[s:], jnp.zeros((s, LANES), F32)], axis=0)

    lane = lax.broadcasted_iota(jnp.int32, (BLOCKS, LANES), 1)
    row = lax.broadcasted_iota(jnp.int32, (BLOCKS, LANES), 0)
    left[inside, :] = groups[0]
    right[inside, :] = pltpu.roll(groups[0], LANES - TILES, 1)
    value[inside, :] = groups[2]
    u = jnp.where(row == 0, 0.0, pltpu.roll(groups[0], LANES - 2 * TILES, 1))
    v = jnp.where(row == BLOCKS - 1, 0.0, pltpu.roll(groups[0], LANES - 3 * TILES, 1))
    w = pltpu.roll(groups[2], LANES - TILES, 1)
    r = 1.0 / (1.0 - v * high(None, left, 1))
    e = u * r
    f = v * high(None, right, 1) * r
    d = (w + v * high(None, value, 1)) * r
    s = 1
    while s < BLOCKS:
        if s < SUB:
            left[inside, :] = e
            right[inside, :] = f
            value[inside, :] = d
        r = 1.0 / (1.0 - e * low(f, right, s) - f * high(e, left, s))
        d = (d + e * low(d, value, s) + f * high(d, value, s)) * r
        if 2 * s < BLOCKS:
            e, f = e * low(e, left, s) * r, f * high(f, right, s) * r
        s *= 2
    z = d
    for g in range(1, 4):
        z = jnp.where(lane >= g * TILES, pltpu.roll(d, g * TILES, 1), z)
    value[inside, :] = z
    x = low(None, value, 1)
    part = lane[:1] // TILES
    square = groups[1] * jnp.where(
        lane < TILES, x, jnp.where(lane < 2 * TILES, z, x * jnp.where(lane < 3 * TILES, x, z))
    )
    cross = groups[3] * jnp.where(lane < TILES, x, jnp.where(lane < 2 * TILES, z, z * z))

    def rows(y):
        return jnp.sum(y, axis=0, keepdims=True)

    square, cross, plain = rows(square), rows(cross), rows(groups[2])
    mass = jnp.where(part < 2, square, jnp.where(part == 2, plain, 0.0))
    error = (
        jnp.where(part == 2, square, jnp.where(part == 3, 2.0 * square + plain, 0.0))
        + jnp.where(part < 2, 2.0 * cross, jnp.where(part == 2, cross, 0.0))
    )
    mass = jnp.sum(mass, axis=1, keepdims=True)
    error = jnp.sum(error, axis=1, keepdims=True)
    totals = jnp.where(part == 2, mass, error)
    back[...] = jnp.where(
        lane < TILES, z, jnp.where(lane < 2 * TILES, x, jnp.broadcast_to(totals, (BLOCKS, LANES)))
    )


def final_kernel(got, part, above, below, update, totals, lines):
    t = got[...].T
    z = t[:TILES]
    x = t[TILES:2 * TILES]
    scale = 1.0 / (BLOCKS * ROWS * NY)
    totals[0] = jnp.sum(t[2 * TILES:2 * TILES + 1]) * scale
    totals[1] = jnp.sum(t[3 * TILES:3 * TILES + 1]) * scale
    for r in range(INNER):
        lines[line(r), :] = part[wide(r), :] + above[wide(r), :] * x + below[wide(r), :] * z
    lines[line(INNER), :] = z
    for h in range(HALVES):
        for i in range(TILES):
            update[h * SUB:(h + 1) * SUB, i * LANES:(i + 1) * LANES] = lines[tile(h, i), :]


def body(history, source, diffusivity, target):
    anywhere = pl.BlockSpec(memory_space=pltpu.HBM)
    vmem = pl.BlockSpec(memory_space=pltpu.VMEM)
    shape = jax.ShapeDtypeStruct
    block = pltpu.VMEM((ROWS, NY), F32)
    tiles = pltpu.VMEM((VREGS * SUB, LANES), F32)
    pair = pltpu.VMEM((2, VREGS * SUB, LANES), F32)
    stages = pltpu.VMEM((STEPS + 1, VREGS * SUB, LANES), F32)
    block_tile = pltpu.VMEM((ROWS, LANES), F32)
    lines = INNER * TILES
    params = pltpu.CompilerParams(vmem_limit_bytes=48 * 1024 * 1024)
    msg, part, above, below = pl.pallas_call(
        local_kernel,
        name="local",
        out_shape=[shape((4 * BLOCKS, LANES), F32)] + [shape((lines, LANES), F32)] * 3,
        in_specs=[anywhere] * 4,
        out_specs=[vmem] * 4,
        scratch_shapes=[
            pltpu.VMEM((LEVELS, ROWS, NY), F32), block, block, block,
            stages, stages, pair, tiles, tiles, tiles, block_tile, pair,
            tiles, tiles, tiles, tiles, tiles, tiles, tiles,
            pltpu.VMEM((LEVELS * SUB, LANES), F32),
            pltpu.SemaphoreType.DMA((3 + HALVES * CHUNKS,)),
        ],
        compiler_params=params,
    )(*(pltpu.with_memory_space_constraint(x, pltpu.HBM) for x in (history, source, diffusivity, target)))
    got = lax.all_to_all(
        msg.reshape(BLOCKS, 4, LANES), AXIS, split_axis=0, concat_axis=0, tiled=True
    ).reshape(4 * BLOCKS, LANES)
    back = pl.pallas_call(
        reduced_kernel,
        name="reduced",
        out_shape=shape((BLOCKS, LANES), F32),
        in_specs=[vmem],
        out_specs=vmem,
        scratch_shapes=[pltpu.VMEM((BLOCKS + 2 * SUB, LANES), F32)] * 3,
        compiler_params=params,
    )(got)
    solved = lax.all_to_all(back, AXIS, split_axis=0, concat_axis=0, tiled=True)
    return pl.pallas_call(
        final_kernel,
        name="final",
        out_shape=[shape((ROWS, NY), F32), shape((2,), F32)],
        in_specs=[vmem] * 4,
        out_specs=[vmem, pl.BlockSpec(memory_space=pltpu.SMEM)],
        scratch_shapes=[tiles],
        compiler_params=params,
    )(solved, part, above, below)


def solution(mesh):
    return jax.shard_map(
        body,
        mesh=mesh,
        in_specs=(P(None, AXIS, None), P(AXIS, None), P(AXIS, None), P(AXIS, None)),
        out_specs=(P(AXIS, None), P()),
        check_vma=False,
    )
```

```python
import jax
import jax.numpy as jnp
import numpy as np
from jax import lax
from jax.experimental import pallas as pl
from jax.experimental.pallas import tpu as pltpu
from jax.sharding import PartitionSpec as P

STIFF = 1024.0
ORDER = 0.6
AXIS = "rows"
LANES = 128
SUB = 8
LEVELS = 32
ROWS = 16
NY = 4096
TILES = NY // LANES
HALVES = ROWS // SUB
VREGS = HALVES * TILES
BLOCKS = 128
INNER = ROWS - 1
CHUNK_TILES = 8
PIECES = ((0, 16, 32), (0, 16, 32))
COPIES = 3 + sum(len(cuts) - 1 for cuts in PIECES)
STEPS = 7
MID = TILES // 2
F32 = jnp.float32


def history_weights():
    moments = np.arange(LEVELS + 1, dtype=np.float64) ** (1.0 - ORDER)
    b = moments[1:] - moments[:-1]
    w = np.concatenate([b[1:], [0.0]]) - np.concatenate([[0.0], b[1:]])
    scale = -w
    scale[0] = 1.0 - w[0]
    return [float(v) for v in scale.astype(np.float32)]


def tile(h, t):
    return pl.ds((h * TILES + t % TILES) * SUB, SUB)


def line(r):
    return pl.ds((r // SUB) * TILES * SUB + r % SUB, TILES, stride=SUB)


def wide(r):
    return pl.ds(r * TILES, TILES)


def lows(load, stride, lane):
    before = pltpu.roll(load(TILES - 1), stride, 1)
    for t in range(TILES):
        down = pltpu.roll(load(t), stride, 1)
        yield jnp.where(lane < stride, before, down)
        before = down


def highs(load, stride, lane):
    back = LANES - stride
    first = here = pltpu.roll(load(0), back, 1)
    for t in range(TILES):
        after = first if t == TILES - 1 else pltpu.roll(load(t + 1), back, 1)
        yield jnp.where(lane >= back, after, here)
        here = after


def both(load, lane):
    half = LANES // 2
    last = before = pltpu.roll(load(TILES - 1), half, 1)
    first = here = pltpu.roll(load(0), half, 1)
    for t in range(TILES):
        if t == TILES - 1:
            after = first
        elif t == TILES - 2:
            after = last
        else:
            after = pltpu.roll(load(t + 1), half, 1)
        yield jnp.where(lane < half, before, here), jnp.where(lane >= half, after, here)
        before, here = here, after


def local_kernel(
    hist_hbm, src_hbm, dif_hbm, tgt_hbm,
    msg, part, above, below,
    hist, src, dif, tgt,
    couple, inv, main, upper, beyond, first, centre, rhs,
    dif_l, tgt_l, sw_l, gg, hh, rr, pp,
    weights, sems,
):
    def piece(h, k, sem):
        rows = pl.ds(h * SUB, SUB)
        cols = pl.ds(PIECES[h][k] * LANES, (PIECES[h][k + 1] - PIECES[h][k]) * LANES)
        return pltpu.make_async_copy(hist_hbm.at[:, rows, cols], hist.at[:, rows, cols], sem)

    copies = [
        pltpu.make_async_copy(dif_hbm, dif, sems.at[0]),
        pltpu.make_async_copy(src_hbm, src, sems.at[1]),
        pltpu.make_async_copy(tgt_hbm, tgt, sems.at[2]),
    ]
    pieces = []
    for h in range(HALVES):
        pieces.append([])
        for k in range(len(PIECES[h]) - 1):
            copies.append(piece(h, k, sems.at[len(copies)]))
            pieces[h].append(copies[-1])
    for copy in [*copies[:2], *pieces[0], copies[2], *pieces[1]]:
        copy.start()
    lane = lax.broadcasted_iota(jnp.int32, (SUB, LANES), 1)
    for k, value in enumerate(history_weights()):
        weights[pl.ds(k * SUB, SUB), :] = jnp.full((SUB, LANES), value, F32)

    copies[0].wait()
    for h in range(HALVES):
        for t in range(TILES):
            c = STIFF * dif[h * SUB:(h + 1) * SUB, t * LANES:(t + 1) * LANES]
            dif_l[tile(h, t), :] = c
            q = 1.0 / c
            first[tile(h, t), :] = q
            u = 0.5 * q * (1.0 / (2.0 + q))
            couple[0, tile(h, t), :] = u
            inv[0, tile(h, t), :] = 0.5 - u

    g = h_ = None
    for r in range(ROWS):
        c = dif_l[line(r), :]
        if r == 0:
            q = 1.0 / (1.0 + 2.0 * c)
            g = c * q
            h_ = g
        else:
            q = 1.0 / (1.0 + 2.0 * c - c * g)
            g = c * q
            h_ = g * h_
        rr[wide(r), :] = q
        gg[wide(r), :] = g
        hh[wide(r), :] = h_
    a = hh[wide(INNER - 1), :]
    b = gg[wide(INNER - 1), :]
    zero = jnp.zeros((TILES, LANES), F32)
    sum_a = sum_b = sum_aa = sum_ab = sum_bb = zero
    for r in reversed(range(INNER)):
        if r < INNER - 1:
            g = gg[wide(r), :]
            a = hh[wide(r), :] + g * a
            b = g * b
        above[wide(r), :] = a
        below[wide(r), :] = b
        sum_a = sum_a + a
        sum_b = sum_b + b
        sum_aa = sum_aa + a * a
        sum_ab = sum_ab + a * b
        sum_bb = sum_bb + b * b
    def send(group, four):
        stacked = jnp.concatenate(four, axis=0)
        msg[pl.ds(group, BLOCKS, stride=4), :] = stacked.T

    send(0, [a, b, hh[wide(INNER), :], gg[wide(INNER), :]])
    send(1, [sum_a, sum_b + 1.0, sum_aa, sum_ab])

    def bands(h):
        low_u = lows(lambda t: couple[0, tile(h, t), :], 1, lane)
        high_u = highs(lambda t: couple[0, tile(h, t), :], 1, lane)
        for t in range(TILES):
            low = next(low_u)
            high = next(high_u)
            q = first[tile(h, t), :]
            m = 1.0 + (q + low + high)
            b = 0.5 - low
            if t == 0:
                m = jnp.where(lane == 0, 1.5 + (q + high), m)
                b = jnp.where(lane < 2, 0.0, b)
            if t == TILES - 1:
                m = jnp.where(lane == LANES - 1, 1.5 + (q + low), m)
            main[1, tile(h, t), :] = m
            couple[1, tile(h, t), :] = b
            inv[1, tile(h, t), :] = 1.0 / m
            yield
        for k in range(1, STEPS):
            stride = 1 << k
            now = k % 2

            def v_of(t):
                return inv[k, tile(h, t), :]

            def p_of(t):
                return couple[k, tile(h, t), :] * v_of(t)

            if k == STEPS - 1:
                pairs_v = both(v_of, lane)
                pairs_b = both(lambda t: couple[k, tile(h, t), :], lane)
                for t in range(TILES):
                    b = couple[k, tile(h, t), :]
                    low_v, high_v = next(pairs_v)
                    low_b, high_b = next(pairs_b)
                    beyond[tile(h, t), :] = high_b
                    m = main[now, tile(h, t), :] - b * b * low_v - high_b * high_b * high_v
                    main[1 - now, tile(h, t), :] = m
                    couple[k + 1, tile(h, t), :] = b * low_b * low_v
                    yield
                continue
            low_v = lows(v_of, stride, lane)
            low_p = lows(p_of, stride, lane)
            high_s = highs(lambda t: couple[k, tile(h, t), :] * p_of(t), stride, lane)
            for t in range(TILES):
                b = couple[k, tile(h, t), :]
                m = main[now, tile(h, t), :] - b * b * next(low_v) - next(high_s)
                main[1 - now, tile(h, t), :] = m
                couple[k + 1, tile(h, t), :] = b * next(low_p)
                inv[k + 1, tile(h, t), :] = 1.0 / m
                yield
        a = b = 0.0
        below_b = couple[STEPS, tile(h, 0), :]
        ends = [below_b]
        for step in range(MID):
            t = step
            e = ends.pop()
            f = couple[STEPS, tile(h, t + 1), :]
            ends.append(f)
            q = 1.0 / (main[STEPS % 2, tile(h, t), :] - e * b)
            inv[STEPS, tile(h, t), :] = q
            couple[STEPS, tile(h, t), :] = e * q
            b = f * q
            upper[tile(h, t), :] = b
            t = TILES - 1 - step
            e = couple[STEPS, tile(h, t), :]
            f = below_b
            below_b = e
            q = 1.0 / (main[STEPS % 2, tile(h, t), :] - f * a)
            inv[STEPS, tile(h, t), :] = q
            a = e * q
            couple[STEPS, tile(h, t), :] = a
            upper[tile(h, t), :] = f * q
            yield
        centre[pl.ds(h * SUB, SUB), :] = 1.0 / (1.0 - b * a)

    def drive(h, c):
        rows = slice(h * SUB, (h + 1) * SUB)
        own = range(c * CHUNK_TILES, (c + 1) * CHUNK_TILES)
        acc = [src[rows, t * LANES:(t + 1) * LANES] for t in own]
        for k in range(LEVELS):
            weight = weights[pl.ds(k * SUB, SUB), :]
            for i, t in enumerate(own):
                acc[i] = acc[i] + weight * hist[k, rows, t * LANES:(t + 1) * LANES]
        for i, t in enumerate(own):
            rhs[0, tile(h, t), :] = acc[i] * first[tile(h, t), :]

    def right_side(h):
        for k in range(STEPS):
            now = k % 2

            def z_of(t):
                return inv[k, tile(h, t), :] * rhs[now, tile(h, t), :]

            def y_of(t):
                return z_of(t) if k == 0 else couple[k, tile(h, t), :] * z_of(t)

            if k == STEPS - 1:
                pairs_z = both(z_of, lane)
                for t in range(TILES):
                    low, high = next(pairs_z)
                    low = couple[k, tile(h, t), :] * low
                    high = beyond[tile(h, t), :] * high
                    rhs[1 - now, tile(h, t), :] = rhs[now, tile(h, t), :] + low + high
                continue
            low_z = lows(z_of, 1 << k, lane)
            high_y = highs(y_of, 1 << k, lane)
            for t in range(TILES):
                low = next(low_z)
                high = next(high_y)
                if k:
                    low = couple[k, tile(h, t), :] * low
                elif t == 0:
                    low = jnp.where(lane == 0, 0.0, low)
                elif t == TILES - 1:
                    high = jnp.where(lane == LANES - 1, 0.0, high)
                rhs[1 - now, tile(h, t), :] = rhs[now, tile(h, t), :] + low + high
        d = [inv[STEPS, tile(h, t), :] * rhs[STEPS % 2, tile(h, t), :] for t in range(TILES)]
        for step in range(1, MID):
            t = step
            d[t] = d[t] + couple[STEPS, tile(h, t), :] * d[t - 1]
            t = TILES - 1 - step
            d[t] = d[t] + upper[tile(h, t), :] * d[t + 1]
        x = d[MID - 1] + upper[tile(h, MID - 1), :] * d[MID]
        x = x * centre[pl.ds(h * SUB, SUB), :]
        y = d[MID] + couple[STEPS, tile(h, MID), :] * x
        sw_l[tile(h, MID - 1), :] = x
        sw_l[tile(h, MID), :] = y
        for step in range(1, MID):
            t = MID - 1 - step
            x = d[t] + upper[tile(h, t), :] * x
            sw_l[tile(h, t), :] = x
            t = MID + step
            y = d[t] + couple[STEPS, tile(h, t), :] * y
            sw_l[tile(h, t), :] = y

    halves = [bands(h) for h in range(HALVES)]
    for k in range(STEPS + 1):
        for half in halves:
            for _ in range(TILES):
                next(half, None)

    copies[1].wait()
    p = None
    for h in range(HALVES):
        if h == HALVES - 1:
            copies[2].wait()
            for i in range(VREGS):
                g = i // TILES
                t = i % TILES
                tgt_l[tile(g, t), :] = tgt[g * SUB:(g + 1) * SUB, t * LANES:(t + 1) * LANES]
        for c in range(TILES // CHUNK_TILES):
            if c * CHUNK_TILES in PIECES[h]:
                pieces[h][PIECES[h].index(c * CHUNK_TILES)].wait()
            drive(h, c)
        right_side(h)
        for r in range(h * SUB, (h + 1) * SUB):
            s = rr[wide(r), :] * sw_l[line(r), :]
            p = s if r == 0 else s + gg[wide(r), :] * p
            pp[wide(r), :] = p
    tip = p
    d = tgt_l[line(INNER), :]
    sum_dd = d * d
    sum_db = -d
    sum_da = zero
    sum_p = zero
    p = pp[wide(INNER - 1), :]
    for r in reversed(range(INNER)):
        if r < INNER - 1:
            p = pp[wide(r), :] + gg[wide(r), :] * p
        part[wide(r), :] = p
        a = above[wide(r), :]
        b = below[wide(r), :]
        d = p - tgt_l[line(r), :]
        sum_p = sum_p + p
        sum_dd = sum_dd + d * d
        sum_da = sum_da + d * a
        sum_db = sum_db + d * b
    send(2, [p, tip, sum_p, sum_dd])
    send(3, [sum_da, sum_db, sum_bb + 1.0, zero])


def reduced_kernel(got, back, left, right, value):
    groups = [got[pl.ds(g, BLOCKS, stride=4), :] for g in range(4)]
    edge = jnp.zeros((SUB, LANES), F32)
    for ref in (left, right, value):
        ref[pl.ds(0, SUB), :] = edge
        ref[pl.ds(SUB + BLOCKS, SUB), :] = edge
    inside = pl.ds(SUB, BLOCKS)

    def low(x, ref, s):
        if s < SUB:
            return ref[pl.ds(SUB - s, BLOCKS), :]
        return jnp.concatenate([jnp.zeros((s, LANES), F32), x[:BLOCKS - s]], axis=0)

    def high(x, ref, s):
        if s < SUB:
            return ref[pl.ds(SUB + s, BLOCKS), :]
        return jnp.concatenate([x[s:], jnp.zeros((s, LANES), F32)], axis=0)

    lane = lax.broadcasted_iota(jnp.int32, (BLOCKS, LANES), 1)
    row = lax.broadcasted_iota(jnp.int32, (BLOCKS, LANES), 0)
    left[inside, :] = groups[0]
    right[inside, :] = pltpu.roll(groups[0], LANES - TILES, 1)
    value[inside, :] = groups[2]
    u = jnp.where(row == 0, 0.0, pltpu.roll(groups[0], LANES - 2 * TILES, 1))
    v = jnp.where(row == BLOCKS - 1, 0.0, pltpu.roll(groups[0], LANES - 3 * TILES, 1))
    w = pltpu.roll(groups[2], LANES - TILES, 1)
    r = 1.0 / (1.0 - v * high(None, left, 1))
    e = u * r
    f = v * high(None, right, 1) * r
    d = (w + v * high(None, value, 1)) * r
    s = 1
    while s < BLOCKS:
        if s < SUB:
            left[inside, :] = e
            right[inside, :] = f
            value[inside, :] = d
        r = 1.0 / (1.0 - e * low(f, right, s) - f * high(e, left, s))
        d = (d + e * low(d, value, s) + f * high(d, value, s)) * r
        if 2 * s < BLOCKS:
            e, f = e * low(e, left, s) * r, f * high(f, right, s) * r
        s *= 2
    z = d
    for g in range(1, 4):
        z = jnp.where(lane >= g * TILES, pltpu.roll(d, g * TILES, 1), z)
    value[inside, :] = z
    x = low(None, value, 1)
    part = lane[:1] // TILES
    square = groups[1] * jnp.where(
        lane < TILES, x, jnp.where(lane < 2 * TILES, z, x * jnp.where(lane < 3 * TILES, x, z))
    )
    cross = groups[3] * jnp.where(lane < TILES, x, jnp.where(lane < 2 * TILES, z, z * z))

    def rows(y):
        return jnp.sum(y, axis=0, keepdims=True)

    square, cross, plain = rows(square), rows(cross), rows(groups[2])
    mass = jnp.where(part < 2, square, jnp.where(part == 2, plain, 0.0))
    error = (
        jnp.where(part == 2, square, jnp.where(part == 3, 2.0 * square + plain, 0.0))
        + jnp.where(part < 2, 2.0 * cross, jnp.where(part == 2, cross, 0.0))
    )
    mass = jnp.sum(mass, axis=1, keepdims=True)
    error = jnp.sum(error, axis=1, keepdims=True)
    totals = jnp.where(part == 2, mass, error)
    back[...] = jnp.where(
        lane < TILES, z, jnp.where(lane < 2 * TILES, x, jnp.broadcast_to(totals, (BLOCKS, LANES)))
    )


def final_kernel(got, part, above, below, update, totals):
    t = got[...].T
    z = t[:TILES]
    x = t[TILES:2 * TILES]
    scale = 1.0 / (BLOCKS * ROWS * NY)
    totals[0] = jnp.sum(t[2 * TILES:2 * TILES + 1]) * scale
    totals[1] = jnp.sum(t[3 * TILES:3 * TILES + 1]) * scale
    for r in range(INNER):
        update[line(r), :] = part[wide(r), :] + above[wide(r), :] * x + below[wide(r), :] * z
    update[line(INNER), :] = z


def body(history, source, diffusivity, target):
    anywhere = pl.BlockSpec(memory_space=pltpu.HBM)
    vmem = pl.BlockSpec(memory_space=pltpu.VMEM)
    shape = jax.ShapeDtypeStruct
    block = pltpu.VMEM((ROWS, NY), F32)
    tiles = pltpu.VMEM((VREGS * SUB, LANES), F32)
    pair = pltpu.VMEM((2, VREGS * SUB, LANES), F32)
    stages = pltpu.VMEM((STEPS + 1, VREGS * SUB, LANES), F32)
    block_tile = pltpu.VMEM((ROWS, LANES), F32)
    lines = INNER * TILES
    params = pltpu.CompilerParams(vmem_limit_bytes=48 * 1024 * 1024)
    msg, part, above, below = pl.pallas_call(
        local_kernel,
        name="local",
        out_shape=[shape((4 * BLOCKS, LANES), F32)] + [shape((lines, LANES), F32)] * 3,
        in_specs=[anywhere] * 4,
        out_specs=[vmem] * 4,
        scratch_shapes=[
            pltpu.VMEM((LEVELS, ROWS, NY), F32), block, block, block,
            stages, stages, pair, tiles, tiles, tiles, block_tile, pair,
            tiles, tiles, tiles, tiles, tiles, tiles, tiles,
            pltpu.VMEM((LEVELS * SUB, LANES), F32),
            pltpu.SemaphoreType.DMA((COPIES,)),
        ],
        compiler_params=params,
    )(*(pltpu.with_memory_space_constraint(x, pltpu.HBM) for x in (history, source, diffusivity, target)))
    got = lax.all_to_all(
        msg.reshape(BLOCKS, 4, LANES), AXIS, split_axis=0, concat_axis=0, tiled=True
    ).reshape(4 * BLOCKS, LANES)
    back = pl.pallas_call(
        reduced_kernel,
        name="reduced",
        out_shape=shape((BLOCKS, LANES), F32),
        in_specs=[vmem],
        out_specs=vmem,
        scratch_shapes=[pltpu.VMEM((BLOCKS + 2 * SUB, LANES), F32)] * 3,
        compiler_params=params,
    )(got)
    solved = lax.all_to_all(back, AXIS, split_axis=0, concat_axis=0, tiled=True)
    update, totals = pl.pallas_call(
        final_kernel,
        name="final",
        out_shape=[shape((VREGS * SUB, LANES), F32), shape((2,), F32)],
        in_specs=[vmem] * 4,
        out_specs=[vmem, pl.BlockSpec(memory_space=pltpu.SMEM)],
        compiler_params=params,
    )(solved, part, above, below)
    update = update.reshape(HALVES, TILES, SUB, LANES).transpose(0, 2, 1, 3).reshape(ROWS, NY)
    return update, totals


def solution(mesh):
    return jax.shard_map(
        body,
        mesh=mesh,
        in_specs=(P(None, AXIS, None), P(AXIS, None), P(AXIS, None), P(AXIS, None)),
        out_specs=(P(AXIS, None), P()),
        check_vma=False,
    )
```

```python
import jax
import jax.numpy as jnp
import numpy as np
from jax import lax
from jax.experimental import pallas as pl
from jax.experimental.pallas import tpu as pltpu
from jax.sharding import PartitionSpec as P

STIFF = 1024.0
ORDER = 0.6
AXIS = "rows"
LANES = 128
SUB = 8
LEVELS = 32
ROWS = 16
NY = 4096
TILES = NY // LANES
HALVES = ROWS // SUB
VREGS = HALVES * TILES
BLOCKS = 128
INNER = ROWS - 1
CHUNK_TILES = 8
PIECES = ((0, 16, 32), (0, 16, 32))
COPIES = 3 + sum(len(cuts) - 1 for cuts in PIECES)
STEPS = 7
MID = TILES // 2
F32 = jnp.float32


def history_weights():
    moments = np.arange(LEVELS + 1, dtype=np.float64) ** (1.0 - ORDER)
    b = moments[1:] - moments[:-1]
    w = np.concatenate([b[1:], [0.0]]) - np.concatenate([[0.0], b[1:]])
    scale = -w
    scale[0] = 1.0 - w[0]
    return [float(v) for v in scale.astype(np.float32)]


def tile(h, t):
    return pl.ds((h * TILES + t % TILES) * SUB, SUB)


def line(r):
    return pl.ds((r // SUB) * TILES * SUB + r % SUB, TILES, stride=SUB)


def wide(r):
    return pl.ds(r * TILES, TILES)


def lows(load, stride, lane):
    before = pltpu.roll(load(TILES - 1), stride, 1)
    for t in range(TILES):
        down = pltpu.roll(load(t), stride, 1)
        yield jnp.where(lane < stride, before, down)
        before = down


def highs(load, stride, lane):
    back = LANES - stride
    first = here = pltpu.roll(load(0), back, 1)
    for t in range(TILES):
        after = first if t == TILES - 1 else pltpu.roll(load(t + 1), back, 1)
        yield jnp.where(lane >= back, after, here)
        here = after


def both(load, lane):
    half = LANES // 2
    last = before = pltpu.roll(load(TILES - 1), half, 1)
    first = here = pltpu.roll(load(0), half, 1)
    for t in range(TILES):
        if t == TILES - 1:
            after = first
        elif t == TILES - 2:
            after = last
        else:
            after = pltpu.roll(load(t + 1), half, 1)
        yield jnp.where(lane < half, before, here), jnp.where(lane >= half, after, here)
        before, here = here, after


def local_kernel(
    hist_hbm, src_hbm, dif_hbm, tgt_hbm,
    msg, part, above, below,
    hist, src, dif, tgt,
    couple, inv, main, upper, beyond, first, centre, rhs,
    sw_l, gg, hh, rr, pp,
    weights, sems,
):
    def piece(h, k, sem):
        rows = pl.ds(h * SUB, SUB)
        cols = pl.ds(PIECES[h][k] * LANES, (PIECES[h][k + 1] - PIECES[h][k]) * LANES)
        return pltpu.make_async_copy(hist_hbm.at[:, rows, cols], hist.at[:, rows, cols], sem)

    copies = [
        pltpu.make_async_copy(dif_hbm, dif, sems.at[0]),
        pltpu.make_async_copy(src_hbm, src, sems.at[1]),
        pltpu.make_async_copy(tgt_hbm, tgt, sems.at[2]),
    ]
    pieces = []
    for h in range(HALVES):
        pieces.append([])
        for k in range(len(PIECES[h]) - 1):
            copies.append(piece(h, k, sems.at[len(copies)]))
            pieces[h].append(copies[-1])
    for copy in [*copies[:2], *pieces[0], copies[2], *pieces[1]]:
        copy.start()
    lane = lax.broadcasted_iota(jnp.int32, (SUB, LANES), 1)
    for k, value in enumerate(history_weights()):
        weights[pl.ds(k * SUB, SUB), :] = jnp.full((SUB, LANES), value, F32)

    copies[0].wait()
    for h in range(HALVES):
        for t in range(TILES):
            c = STIFF * dif[tile(h, t), :]
            q = 1.0 / c
            first[tile(h, t), :] = q
            u = 0.5 * q * (1.0 / (2.0 + q))
            couple[0, tile(h, t), :] = u
            inv[0, tile(h, t), :] = 0.5 - u

    g = h_ = None
    for r in range(ROWS):
        c = STIFF * dif[line(r), :]
        if r == 0:
            q = 1.0 / (1.0 + 2.0 * c)
            g = c * q
            h_ = g
        else:
            q = 1.0 / (1.0 + 2.0 * c - c * g)
            g = c * q
            h_ = g * h_
        rr[wide(r), :] = q
        gg[wide(r), :] = g
        hh[wide(r), :] = h_
    a = hh[wide(INNER - 1), :]
    b = gg[wide(INNER - 1), :]
    zero = jnp.zeros((TILES, LANES), F32)
    sum_a = sum_b = sum_aa = sum_ab = sum_bb = zero
    for r in reversed(range(INNER)):
        if r < INNER - 1:
            g = gg[wide(r), :]
            a = hh[wide(r), :] + g * a
            b = g * b
        above[wide(r), :] = a
        below[wide(r), :] = b
        sum_a = sum_a + a
        sum_b = sum_b + b
        sum_aa = sum_aa + a * a
        sum_ab = sum_ab + a * b
        sum_bb = sum_bb + b * b
    def send(group, four):
        stacked = jnp.concatenate(four, axis=0)
        msg[pl.ds(group, BLOCKS, stride=4), :] = stacked.T

    send(0, [a, b, hh[wide(INNER), :], gg[wide(INNER), :]])
    send(1, [sum_a, sum_b + 1.0, sum_aa, sum_ab])

    def bands(h):
        low_u = lows(lambda t: couple[0, tile(h, t), :], 1, lane)
        high_u = highs(lambda t: couple[0, tile(h, t), :], 1, lane)
        for t in range(TILES):
            low = next(low_u)
            high = next(high_u)
            q = first[tile(h, t), :]
            m = 1.0 + (q + low + high)
            b = 0.5 - low
            if t == 0:
                m = jnp.where(lane == 0, 1.5 + (q + high), m)
                b = jnp.where(lane < 2, 0.0, b)
            if t == TILES - 1:
                m = jnp.where(lane == LANES - 1, 1.5 + (q + low), m)
            main[1, tile(h, t), :] = m
            couple[1, tile(h, t), :] = b
            inv[1, tile(h, t), :] = 1.0 / m
            yield
        for k in range(1, STEPS):
            stride = 1 << k
            now = k % 2

            def v_of(t):
                return inv[k, tile(h, t), :]

            def p_of(t):
                return couple[k, tile(h, t), :] * v_of(t)

            if k == STEPS - 1:
                pairs_v = both(v_of, lane)
                pairs_b = both(lambda t: couple[k, tile(h, t), :], lane)
                for t in range(TILES):
                    b = couple[k, tile(h, t), :]
                    low_v, high_v = next(pairs_v)
                    low_b, high_b = next(pairs_b)
                    beyond[tile(h, t), :] = high_b
                    m = main[now, tile(h, t), :] - b * b * low_v - high_b * high_b * high_v
                    main[1 - now, tile(h, t), :] = m
                    couple[k + 1, tile(h, t), :] = b * low_b * low_v
                    yield
                continue
            low_v = lows(v_of, stride, lane)
            low_p = lows(p_of, stride, lane)
            high_s = highs(lambda t: couple[k, tile(h, t), :] * p_of(t), stride, lane)
            for t in range(TILES):
                b = couple[k, tile(h, t), :]
                m = main[now, tile(h, t), :] - b * b * next(low_v) - next(high_s)
                main[1 - now, tile(h, t), :] = m
                couple[k + 1, tile(h, t), :] = b * next(low_p)
                inv[k + 1, tile(h, t), :] = 1.0 / m
                yield
        a = b = 0.0
        below_b = couple[STEPS, tile(h, 0), :]
        ends = [below_b]
        for step in range(MID):
            t = step
            e = ends.pop()
            f = couple[STEPS, tile(h, t + 1), :]
            ends.append(f)
            q = 1.0 / (main[STEPS % 2, tile(h, t), :] - e * b)
            inv[STEPS, tile(h, t), :] = q
            couple[STEPS, tile(h, t), :] = e * q
            b = f * q
            upper[tile(h, t), :] = b
            t = TILES - 1 - step
            e = couple[STEPS, tile(h, t), :]
            f = below_b
            below_b = e
            q = 1.0 / (main[STEPS % 2, tile(h, t), :] - f * a)
            inv[STEPS, tile(h, t), :] = q
            a = e * q
            couple[STEPS, tile(h, t), :] = a
            upper[tile(h, t), :] = f * q
            yield
        centre[pl.ds(h * SUB, SUB), :] = 1.0 / (1.0 - b * a)

    def drive(h, c):
        rows = slice(h * SUB, (h + 1) * SUB)
        own = range(c * CHUNK_TILES, (c + 1) * CHUNK_TILES)
        acc = [src[rows, t * LANES:(t + 1) * LANES] for t in own]
        for k in range(LEVELS):
            weight = weights[pl.ds(k * SUB, SUB), :]
            for i, t in enumerate(own):
                acc[i] = acc[i] + weight * hist[k, rows, t * LANES:(t + 1) * LANES]
        for i, t in enumerate(own):
            rhs[0, tile(h, t), :] = acc[i] * first[tile(h, t), :]

    def right_side(h):
        for k in range(STEPS):
            now = k % 2

            def z_of(t):
                return inv[k, tile(h, t), :] * rhs[now, tile(h, t), :]

            def y_of(t):
                return z_of(t) if k == 0 else couple[k, tile(h, t), :] * z_of(t)

            if k == STEPS - 1:
                pairs_z = both(z_of, lane)
                for t in range(TILES):
                    low, high = next(pairs_z)
                    low = couple[k, tile(h, t), :] * low
                    high = beyond[tile(h, t), :] * high
                    rhs[1 - now, tile(h, t), :] = rhs[now, tile(h, t), :] + low + high
                continue
            low_z = lows(z_of, 1 << k, lane)
            high_y = highs(y_of, 1 << k, lane)
            for t in range(TILES):
                low = next(low_z)
                high = next(high_y)
                if k:
                    low = couple[k, tile(h, t), :] * low
                elif t == 0:
                    low = jnp.where(lane == 0, 0.0, low)
                elif t == TILES - 1:
                    high = jnp.where(lane == LANES - 1, 0.0, high)
                rhs[1 - now, tile(h, t), :] = rhs[now, tile(h, t), :] + low + high
        d = [inv[STEPS, tile(h, t), :] * rhs[STEPS % 2, tile(h, t), :] for t in range(TILES)]
        for step in range(1, MID):
            t = step
            d[t] = d[t] + couple[STEPS, tile(h, t), :] * d[t - 1]
            t = TILES - 1 - step
            d[t] = d[t] + upper[tile(h, t), :] * d[t + 1]
        x = d[MID - 1] + upper[tile(h, MID - 1), :] * d[MID]
        x = x * centre[pl.ds(h * SUB, SUB), :]
        y = d[MID] + couple[STEPS, tile(h, MID), :] * x
        sw_l[tile(h, MID - 1), :] = x
        sw_l[tile(h, MID), :] = y
        for step in range(1, MID):
            t = MID - 1 - step
            x = d[t] + upper[tile(h, t), :] * x
            sw_l[tile(h, t), :] = x
            t = MID + step
            y = d[t] + couple[STEPS, tile(h, t), :] * y
            sw_l[tile(h, t), :] = y

    halves = [bands(h) for h in range(HALVES)]
    for k in range(STEPS + 1):
        for half in halves:
            for _ in range(TILES):
                next(half, None)

    copies[1].wait()
    p = None
    for h in range(HALVES):
        if h == HALVES - 1:
            copies[2].wait()
        for c in range(TILES // CHUNK_TILES):
            if c * CHUNK_TILES in PIECES[h]:
                pieces[h][PIECES[h].index(c * CHUNK_TILES)].wait()
            drive(h, c)
        right_side(h)
        for r in range(h * SUB, (h + 1) * SUB):
            s = rr[wide(r), :] * sw_l[line(r), :]
            p = s if r == 0 else s + gg[wide(r), :] * p
            pp[wide(r), :] = p
    tip = p
    d = tgt[line(INNER), :]
    sum_dd = d * d
    sum_db = -d
    sum_da = zero
    sum_p = zero
    p = pp[wide(INNER - 1), :]
    for r in reversed(range(INNER)):
        if r < INNER - 1:
            p = pp[wide(r), :] + gg[wide(r), :] * p
        part[wide(r), :] = p
        a = above[wide(r), :]
        b = below[wide(r), :]
        d = p - tgt[line(r), :]
        sum_p = sum_p + p
        sum_dd = sum_dd + d * d
        sum_da = sum_da + d * a
        sum_db = sum_db + d * b
    send(2, [p, tip, sum_p, sum_dd])
    send(3, [sum_da, sum_db, sum_bb + 1.0, zero])


def reduced_kernel(got, back, left, right, value):
    groups = [got[pl.ds(g, BLOCKS, stride=4), :] for g in range(4)]
    edge = jnp.zeros((SUB, LANES), F32)
    for ref in (left, right, value):
        ref[pl.ds(0, SUB), :] = edge
        ref[pl.ds(SUB + BLOCKS, SUB), :] = edge
    inside = pl.ds(SUB, BLOCKS)

    def low(x, ref, s):
        if s < SUB:
            return ref[pl.ds(SUB - s, BLOCKS), :]
        return jnp.concatenate([jnp.zeros((s, LANES), F32), x[:BLOCKS - s]], axis=0)

    def high(x, ref, s):
        if s < SUB:
            return ref[pl.ds(SUB + s, BLOCKS), :]
        return jnp.concatenate([x[s:], jnp.zeros((s, LANES), F32)], axis=0)

    lane = lax.broadcasted_iota(jnp.int32, (BLOCKS, LANES), 1)
    row = lax.broadcasted_iota(jnp.int32, (BLOCKS, LANES), 0)
    left[inside, :] = groups[0]
    right[inside, :] = pltpu.roll(groups[0], LANES - TILES, 1)
    value[inside, :] = groups[2]
    u = jnp.where(row == 0, 0.0, pltpu.roll(groups[0], LANES - 2 * TILES, 1))
    v = jnp.where(row == BLOCKS - 1, 0.0, pltpu.roll(groups[0], LANES - 3 * TILES, 1))
    w = pltpu.roll(groups[2], LANES - TILES, 1)
    r = 1.0 / (1.0 - v * high(None, left, 1))
    e = u * r
    f = v * high(None, right, 1) * r
    d = (w + v * high(None, value, 1)) * r
    s = 1
    while s < BLOCKS:
        if s < SUB:
            left[inside, :] = e
            right[inside, :] = f
            value[inside, :] = d
        r = 1.0 / (1.0 - e * low(f, right, s) - f * high(e, left, s))
        d = (d + e * low(d, value, s) + f * high(d, value, s)) * r
        if 2 * s < BLOCKS:
            e, f = e * low(e, left, s) * r, f * high(f, right, s) * r
        s *= 2
    z = d
    for g in range(1, 4):
        z = jnp.where(lane >= g * TILES, pltpu.roll(d, g * TILES, 1), z)
    value[inside, :] = z
    x = low(None, value, 1)
    part = lane[:1] // TILES
    square = groups[1] * jnp.where(
        lane < TILES, x, jnp.where(lane < 2 * TILES, z, x * jnp.where(lane < 3 * TILES, x, z))
    )
    cross = groups[3] * jnp.where(lane < TILES, x, jnp.where(lane < 2 * TILES, z, z * z))

    def rows(y):
        return jnp.sum(y, axis=0, keepdims=True)

    square, cross, plain = rows(square), rows(cross), rows(groups[2])
    mass = jnp.where(part < 2, square, jnp.where(part == 2, plain, 0.0))
    error = (
        jnp.where(part == 2, square, jnp.where(part == 3, 2.0 * square + plain, 0.0))
        + jnp.where(part < 2, 2.0 * cross, jnp.where(part == 2, cross, 0.0))
    )
    mass = jnp.sum(mass, axis=1, keepdims=True)
    error = jnp.sum(error, axis=1, keepdims=True)
    totals = jnp.where(part == 2, mass, error)
    back[...] = jnp.where(
        lane < TILES, z, jnp.where(lane < 2 * TILES, x, jnp.broadcast_to(totals, (BLOCKS, LANES)))
    )


def final_kernel(got, part, above, below, update, totals):
    t = got[...].T
    z = t[:TILES]
    x = t[TILES:2 * TILES]
    scale = 1.0 / (BLOCKS * ROWS * NY)
    totals[0] = jnp.sum(t[2 * TILES:2 * TILES + 1]) * scale
    totals[1] = jnp.sum(t[3 * TILES:3 * TILES + 1]) * scale
    for r in range(INNER):
        update[line(r), :] = part[wide(r), :] + above[wide(r), :] * x + below[wide(r), :] * z
    update[line(INNER), :] = z


def by_tile(x):
    return x.reshape(HALVES, SUB, TILES, LANES).transpose(0, 2, 1, 3).reshape(VREGS * SUB, LANES)


def body(history, source, diffusivity, target):
    anywhere = pl.BlockSpec(memory_space=pltpu.HBM)
    vmem = pl.BlockSpec(memory_space=pltpu.VMEM)
    shape = jax.ShapeDtypeStruct
    block = pltpu.VMEM((ROWS, NY), F32)
    tiles = pltpu.VMEM((VREGS * SUB, LANES), F32)
    pair = pltpu.VMEM((2, VREGS * SUB, LANES), F32)
    stages = pltpu.VMEM((STEPS + 1, VREGS * SUB, LANES), F32)
    block_tile = pltpu.VMEM((ROWS, LANES), F32)
    lines = INNER * TILES
    params = pltpu.CompilerParams(vmem_limit_bytes=48 * 1024 * 1024)
    msg, part, above, below = pl.pallas_call(
        local_kernel,
        name="local",
        out_shape=[shape((4 * BLOCKS, LANES), F32)] + [shape((lines, LANES), F32)] * 3,
        in_specs=[anywhere] * 4,
        out_specs=[vmem] * 4,
        scratch_shapes=[
            pltpu.VMEM((LEVELS, ROWS, NY), F32), block, tiles, tiles,
            stages, stages, pair, tiles, tiles, tiles, block_tile, pair,
            tiles, tiles, tiles, tiles, tiles,
            pltpu.VMEM((LEVELS * SUB, LANES), F32),
            pltpu.SemaphoreType.DMA((COPIES,)),
        ],
        compiler_params=params,
    )(*(pltpu.with_memory_space_constraint(x, pltpu.HBM) for x in (history, source, by_tile(diffusivity), by_tile(target))))
    got = lax.all_to_all(
        msg.reshape(BLOCKS, 4, LANES), AXIS, split_axis=0, concat_axis=0, tiled=True
    ).reshape(4 * BLOCKS, LANES)
    back = pl.pallas_call(
        reduced_kernel,
        name="reduced",
        out_shape=shape((BLOCKS, LANES), F32),
        in_specs=[vmem],
        out_specs=vmem,
        scratch_shapes=[pltpu.VMEM((BLOCKS + 2 * SUB, LANES), F32)] * 3,
        compiler_params=params,
    )(got)
    solved = lax.all_to_all(back, AXIS, split_axis=0, concat_axis=0, tiled=True)
    update, totals = pl.pallas_call(
        final_kernel,
        name="final",
        out_shape=[shape((VREGS * SUB, LANES), F32), shape((2,), F32)],
        in_specs=[vmem] * 4,
        out_specs=[vmem, pl.BlockSpec(memory_space=pltpu.SMEM)],
        compiler_params=params,
    )(solved, part, above, below)
    update = update.reshape(HALVES, TILES, SUB, LANES).transpose(0, 2, 1, 3).reshape(ROWS, NY)
    return update, totals


def solution(mesh):
    return jax.shard_map(
        body,
        mesh=mesh,
        in_specs=(P(None, AXIS, None), P(AXIS, None), P(AXIS, None), P(AXIS, None)),
        out_specs=(P(AXIS, None), P()),
        check_vma=False,
    )
```

```python
import jax
import jax.numpy as jnp
import numpy as np
from jax import lax
from jax.experimental import pallas as pl
from jax.experimental.pallas import tpu as pltpu
from jax.sharding import PartitionSpec as P

STIFF = 1024.0
ORDER = 0.6
AXIS = "rows"
LANES = 128
SUB = 8
LEVELS = 32
ROWS = 16
NY = 4096
TILES = NY // LANES
HALVES = ROWS // SUB
VREGS = HALVES * TILES
BLOCKS = 128
INNER = ROWS - 1
CHUNK_TILES = 8
PIECES = ((0, 32), (0, 16, 32))
COPIES = 3 + sum(len(cuts) - 1 for cuts in PIECES)
STEPS = 7
MID = TILES // 2
F32 = jnp.float32


def history_weights():
    moments = np.arange(LEVELS + 1, dtype=np.float64) ** (1.0 - ORDER)
    b = moments[1:] - moments[:-1]
    w = np.concatenate([b[1:], [0.0]]) - np.concatenate([[0.0], b[1:]])
    scale = -w
    scale[0] = 1.0 - w[0]
    return [float(v) for v in scale.astype(np.float32)]


def tile(h, t):
    return pl.ds((h * TILES + t % TILES) * SUB, SUB)


def line(r):
    return pl.ds((r // SUB) * TILES * SUB + r % SUB, TILES, stride=SUB)


def wide(r):
    return pl.ds(r * TILES, TILES)


def lows(load, stride, lane):
    before = pltpu.roll(load(TILES - 1), stride, 1)
    for t in range(TILES):
        down = pltpu.roll(load(t), stride, 1)
        yield jnp.where(lane < stride, before, down)
        before = down


def highs(load, stride, lane):
    back = LANES - stride
    first = here = pltpu.roll(load(0), back, 1)
    for t in range(TILES):
        after = first if t == TILES - 1 else pltpu.roll(load(t + 1), back, 1)
        yield jnp.where(lane >= back, after, here)
        here = after


def both(load, lane):
    half = LANES // 2
    last = before = pltpu.roll(load(TILES - 1), half, 1)
    first = here = pltpu.roll(load(0), half, 1)
    for t in range(TILES):
        if t == TILES - 1:
            after = first
        elif t == TILES - 2:
            after = last
        else:
            after = pltpu.roll(load(t + 1), half, 1)
        yield jnp.where(lane < half, before, here), jnp.where(lane >= half, after, here)
        before, here = here, after


def local_kernel(
    hist_hbm, src_hbm, dif_hbm, tgt_hbm,
    msg, part, above, below,
    hist, src, dif, tgt,
    couple, inv, main, upper, beyond, first, centre, rhs,
    dif_l, tgt_l, sw_l, gg, hh, rr, pp,
    weights, sems,
):
    def piece(h, k, sem):
        rows = pl.ds(h * SUB, SUB)
        cols = pl.ds(PIECES[h][k] * LANES, (PIECES[h][k + 1] - PIECES[h][k]) * LANES)
        return pltpu.make_async_copy(hist_hbm.at[:, rows, cols], hist.at[:, rows, cols], sem)

    copies = [
        pltpu.make_async_copy(dif_hbm, dif, sems.at[0]),
        pltpu.make_async_copy(src_hbm, src, sems.at[1]),
        pltpu.make_async_copy(tgt_hbm, tgt, sems.at[2]),
    ]
    pieces = []
    for h in range(HALVES):
        pieces.append([])
        for k in range(len(PIECES[h]) - 1):
            copies.append(piece(h, k, sems.at[len(copies)]))
            pieces[h].append(copies[-1])
    for copy in [*copies[:2], *pieces[0], copies[2], *pieces[1]]:
        copy.start()
    lane = lax.broadcasted_iota(jnp.int32, (SUB, LANES), 1)
    for k, value in enumerate(history_weights()):
        weights[pl.ds(k * SUB, SUB), :] = jnp.full((SUB, LANES), value, F32)

    copies[0].wait()
    for h in range(HALVES):
        for t in range(TILES):
            c = STIFF * dif[h * SUB:(h + 1) * SUB, t * LANES:(t + 1) * LANES]
            dif_l[tile(h, t), :] = c
            q = 1.0 / c
            first[tile(h, t), :] = q
            u = 0.5 * q * (1.0 / (2.0 + q))
            couple[0, tile(h, t), :] = u
            inv[0, tile(h, t), :] = 0.5 - u

    g = h_ = None
    for r in range(ROWS):
        c = dif_l[line(r), :]
        if r == 0:
            q = 1.0 / (1.0 + 2.0 * c)
            g = c * q
            h_ = g
        else:
            q = 1.0 / (1.0 + 2.0 * c - c * g)
            g = c * q
            h_ = g * h_
        rr[wide(r), :] = q
        gg[wide(r), :] = g
        hh[wide(r), :] = h_
    a = hh[wide(INNER - 1), :]
    b = gg[wide(INNER - 1), :]
    zero = jnp.zeros((TILES, LANES), F32)
    sum_a = sum_b = sum_aa = sum_ab = sum_bb = zero
    for r in reversed(range(INNER)):
        if r < INNER - 1:
            g = gg[wide(r), :]
            a = hh[wide(r), :] + g * a
            b = g * b
        above[wide(r), :] = a
        below[wide(r), :] = b
        sum_a = sum_a + a
        sum_b = sum_b + b
        sum_aa = sum_aa + a * a
        sum_ab = sum_ab + a * b
        sum_bb = sum_bb + b * b
    def send(group, four):
        stacked = jnp.concatenate(four, axis=0)
        msg[pl.ds(group, BLOCKS, stride=4), :] = stacked.T

    send(0, [a, b, hh[wide(INNER), :], gg[wide(INNER), :]])
    send(1, [sum_a, sum_b + 1.0, sum_aa, sum_ab])

    def bands(h):
        low_u = lows(lambda t: couple[0, tile(h, t), :], 1, lane)
        high_u = highs(lambda t: couple[0, tile(h, t), :], 1, lane)
        for t in range(TILES):
            low = next(low_u)
            high = next(high_u)
            q = first[tile(h, t), :]
            m = 1.0 + (q + low + high)
            b = 0.5 - low
            if t == 0:
                m = jnp.where(lane == 0, 1.5 + (q + high), m)
                b = jnp.where(lane < 2, 0.0, b)
            if t == TILES - 1:
                m = jnp.where(lane == LANES - 1, 1.5 + (q + low), m)
            main[1, tile(h, t), :] = m
            couple[1, tile(h, t), :] = b
            inv[1, tile(h, t), :] = 1.0 / m
            yield
        for k in range(1, STEPS):
            stride = 1 << k
            now = k % 2

            def v_of(t):
                return inv[k, tile(h, t), :]

            def p_of(t):
                return couple[k, tile(h, t), :] * v_of(t)

            if k == STEPS - 1:
                pairs_v = both(v_of, lane)
                pairs_b = both(lambda t: couple[k, tile(h, t), :], lane)
                for t in range(TILES):
                    b = couple[k, tile(h, t), :]
                    low_v, high_v = next(pairs_v)
                    low_b, high_b = next(pairs_b)
                    beyond[tile(h, t), :] = high_b
                    m = main[now, tile(h, t), :] - b * b * low_v - high_b * high_b * high_v
                    main[1 - now, tile(h, t), :] = m
                    couple[k + 1, tile(h, t), :] = b * low_b * low_v
                    yield
                continue
            low_v = lows(v_of, stride, lane)
            low_p = lows(p_of, stride, lane)
            high_s = highs(lambda t: couple[k, tile(h, t), :] * p_of(t), stride, lane)
            for t in range(TILES):
                b = couple[k, tile(h, t), :]
                m = main[now, tile(h, t), :] - b * b * next(low_v) - next(high_s)
                main[1 - now, tile(h, t), :] = m
                couple[k + 1, tile(h, t), :] = b * next(low_p)
                inv[k + 1, tile(h, t), :] = 1.0 / m
                yield
        a = b = 0.0
        below_b = couple[STEPS, tile(h, 0), :]
        ends = [below_b]
        for step in range(MID):
            t = step
            e = ends.pop()
            f = couple[STEPS, tile(h, t + 1), :]
            ends.append(f)
            q = 1.0 / (main[STEPS % 2, tile(h, t), :] - e * b)
            inv[STEPS, tile(h, t), :] = q
            couple[STEPS, tile(h, t), :] = e * q
            b = f * q
            upper[tile(h, t), :] = b
            t = TILES - 1 - step
            e = couple[STEPS, tile(h, t), :]
            f = below_b
            below_b = e
            q = 1.0 / (main[STEPS % 2, tile(h, t), :] - f * a)
            inv[STEPS, tile(h, t), :] = q
            a = e * q
            couple[STEPS, tile(h, t), :] = a
            upper[tile(h, t), :] = f * q
            yield
        centre[pl.ds(h * SUB, SUB), :] = 1.0 / (1.0 - b * a)

    def drive(h, c):
        rows = slice(h * SUB, (h + 1) * SUB)
        own = range(c * CHUNK_TILES, (c + 1) * CHUNK_TILES)
        acc = [src[rows, t * LANES:(t + 1) * LANES] for t in own]
        for k in range(LEVELS):
            weight = weights[pl.ds(k * SUB, SUB), :]
            for i, t in enumerate(own):
                acc[i] = acc[i] + weight * hist[k, rows, t * LANES:(t + 1) * LANES]
        for i, t in enumerate(own):
            rhs[0, tile(h, t), :] = acc[i] * first[tile(h, t), :]

    def right_side(h):
        for k in range(STEPS):
            now = k % 2

            def z_of(t):
                return inv[k, tile(h, t), :] * rhs[now, tile(h, t), :]

            def y_of(t):
                return z_of(t) if k == 0 else couple[k, tile(h, t), :] * z_of(t)

            if k == STEPS - 1:
                pairs_z = both(z_of, lane)
                for t in range(TILES):
                    low, high = next(pairs_z)
                    low = couple[k, tile(h, t), :] * low
                    high = beyond[tile(h, t), :] * high
                    rhs[1 - now, tile(h, t), :] = rhs[now, tile(h, t), :] + low + high
                continue
            low_z = lows(z_of, 1 << k, lane)
            high_y = highs(y_of, 1 << k, lane)
            for t in range(TILES):
                low = next(low_z)
                high = next(high_y)
                if k:
                    low = couple[k, tile(h, t), :] * low
                elif t == 0:
                    low = jnp.where(lane == 0, 0.0, low)
                elif t == TILES - 1:
                    high = jnp.where(lane == LANES - 1, 0.0, high)
                rhs[1 - now, tile(h, t), :] = rhs[now, tile(h, t), :] + low + high
        d = [inv[STEPS, tile(h, t), :] * rhs[STEPS % 2, tile(h, t), :] for t in range(TILES)]
        for step in range(1, MID):
            t = step
            d[t] = d[t] + couple[STEPS, tile(h, t), :] * d[t - 1]
            t = TILES - 1 - step
            d[t] = d[t] + upper[tile(h, t), :] * d[t + 1]
        x = d[MID - 1] + upper[tile(h, MID - 1), :] * d[MID]
        x = x * centre[pl.ds(h * SUB, SUB), :]
        y = d[MID] + couple[STEPS, tile(h, MID), :] * x
        sw_l[tile(h, MID - 1), :] = x
        sw_l[tile(h, MID), :] = y
        for step in range(1, MID):
            t = MID - 1 - step
            x = d[t] + upper[tile(h, t), :] * x
            sw_l[tile(h, t), :] = x
            t = MID + step
            y = d[t] + couple[STEPS, tile(h, t), :] * y
            sw_l[tile(h, t), :] = y

    halves = [bands(h) for h in range(HALVES)]
    for k in range(STEPS + 1):
        for half in halves:
            for _ in range(TILES):
                next(half, None)

    copies[1].wait()
    p = None
    for h in range(HALVES):
        if h == HALVES - 1:
            copies[2].wait()
            for i in range(VREGS):
                g = i // TILES
                t = i % TILES
                tgt_l[tile(g, t), :] = tgt[g * SUB:(g + 1) * SUB, t * LANES:(t + 1) * LANES]
        for c in range(TILES // CHUNK_TILES):
            if c * CHUNK_TILES in PIECES[h]:
                pieces[h][PIECES[h].index(c * CHUNK_TILES)].wait()
            drive(h, c)
        right_side(h)
        for r in range(h * SUB, (h + 1) * SUB):
            s = rr[wide(r), :] * sw_l[line(r), :]
            p = s if r == 0 else s + gg[wide(r), :] * p
            pp[wide(r), :] = p
    tip = p
    d = tgt_l[line(INNER), :]
    sum_dd = d * d
    sum_db = -d
    sum_da = zero
    sum_p = zero
    p = pp[wide(INNER - 1), :]
    for r in reversed(range(INNER)):
        if r < INNER - 1:
            p = pp[wide(r), :] + gg[wide(r), :] * p
        part[wide(r), :] = p
        a = above[wide(r), :]
        b = below[wide(r), :]
        d = p - tgt_l[line(r), :]
        sum_p = sum_p + p
        sum_dd = sum_dd + d * d
        sum_da = sum_da + d * a
        sum_db = sum_db + d * b
    send(2, [p, tip, sum_p, sum_dd])
    send(3, [sum_da, sum_db, sum_bb + 1.0, zero])


def reduced_kernel(got, back, left, right, value):
    groups = [got[pl.ds(g, BLOCKS, stride=4), :] for g in range(4)]
    edge = jnp.zeros((SUB, LANES), F32)
    for ref in (left, right, value):
        ref[pl.ds(0, SUB), :] = edge
        ref[pl.ds(SUB + BLOCKS, SUB), :] = edge
    inside = pl.ds(SUB, BLOCKS)

    def low(x, ref, s):
        if s < SUB:
            return ref[pl.ds(SUB - s, BLOCKS), :]
        return jnp.concatenate([jnp.zeros((s, LANES), F32), x[:BLOCKS - s]], axis=0)

    def high(x, ref, s):
        if s < SUB:
            return ref[pl.ds(SUB + s, BLOCKS), :]
        return jnp.concatenate([x[s:], jnp.zeros((s, LANES), F32)], axis=0)

    lane = lax.broadcasted_iota(jnp.int32, (BLOCKS, LANES), 1)
    row = lax.broadcasted_iota(jnp.int32, (BLOCKS, LANES), 0)
    left[inside, :] = groups[0]
    right[inside, :] = pltpu.roll(groups[0], LANES - TILES, 1)
    value[inside, :] = groups[2]
    u = jnp.where(row == 0, 0.0, pltpu.roll(groups[0], LANES - 2 * TILES, 1))
    v = jnp.where(row == BLOCKS - 1, 0.0, pltpu.roll(groups[0], LANES - 3 * TILES, 1))
    w = pltpu.roll(groups[2], LANES - TILES, 1)
    r = 1.0 / (1.0 - v * high(None, left, 1))
    e = u * r
    f = v * high(None, right, 1) * r
    d = (w + v * high(None, value, 1)) * r
    s = 1
    while s < BLOCKS:
        if s < SUB:
            left[inside, :] = e
            right[inside, :] = f
            value[inside, :] = d
        r = 1.0 / (1.0 - e * low(f, right, s) - f * high(e, left, s))
        d = (d + e * low(d, value, s) + f * high(d, value, s)) * r
        if 2 * s < BLOCKS:
            e, f = e * low(e, left, s) * r, f * high(f, right, s) * r
        s *= 2
    z = d
    for g in range(1, 4):
        z = jnp.where(lane >= g * TILES, pltpu.roll(d, g * TILES, 1), z)
    value[inside, :] = z
    x = low(None, value, 1)
    part = lane[:1] // TILES
    square = groups[1] * jnp.where(
        lane < TILES, x, jnp.where(lane < 2 * TILES, z, x * jnp.where(lane < 3 * TILES, x, z))
    )
    cross = groups[3] * jnp.where(lane < TILES, x, jnp.where(lane < 2 * TILES, z, z * z))

    def rows(y):
        return jnp.sum(y, axis=0, keepdims=True)

    square, cross, plain = rows(square), rows(cross), rows(groups[2])
    mass = jnp.where(part < 2, square, jnp.where(part == 2, plain, 0.0))
    error = (
        jnp.where(part == 2, square, jnp.where(part == 3, 2.0 * square + plain, 0.0))
        + jnp.where(part < 2, 2.0 * cross, jnp.where(part == 2, cross, 0.0))
    )
    mass = jnp.sum(mass, axis=1, keepdims=True)
    error = jnp.sum(error, axis=1, keepdims=True)
    totals = jnp.where(part == 2, mass, error)
    back[...] = jnp.where(
        lane < TILES, z, jnp.where(lane < 2 * TILES, x, jnp.broadcast_to(totals, (BLOCKS, LANES)))
    )


def final_kernel(got, part, above, below, update, totals):
    t = got[...].T
    z = t[:TILES]
    x = t[TILES:2 * TILES]
    scale = 1.0 / (BLOCKS * ROWS * NY)
    totals[0] = jnp.sum(t[2 * TILES:2 * TILES + 1]) * scale
    totals[1] = jnp.sum(t[3 * TILES:3 * TILES + 1]) * scale
    for r in range(INNER):
        update[line(r), :] = part[wide(r), :] + above[wide(r), :] * x + below[wide(r), :] * z
    update[line(INNER), :] = z


def body(history, source, diffusivity, target):
    anywhere = pl.BlockSpec(memory_space=pltpu.HBM)
    vmem = pl.BlockSpec(memory_space=pltpu.VMEM)
    shape = jax.ShapeDtypeStruct
    block = pltpu.VMEM((ROWS, NY), F32)
    tiles = pltpu.VMEM((VREGS * SUB, LANES), F32)
    pair = pltpu.VMEM((2, VREGS * SUB, LANES), F32)
    stages = pltpu.VMEM((STEPS + 1, VREGS * SUB, LANES), F32)
    block_tile = pltpu.VMEM((ROWS, LANES), F32)
    lines = INNER * TILES
    params = pltpu.CompilerParams(vmem_limit_bytes=48 * 1024 * 1024)
    msg, part, above, below = pl.pallas_call(
        local_kernel,
        name="local",
        out_shape=[shape((4 * BLOCKS, LANES), F32)] + [shape((lines, LANES), F32)] * 3,
        in_specs=[anywhere] * 4,
        out_specs=[vmem] * 4,
        scratch_shapes=[
            pltpu.VMEM((LEVELS, ROWS, NY), F32), block, block, block,
            stages, stages, pair, tiles, tiles, tiles, block_tile, pair,
            tiles, tiles, tiles, tiles, tiles, tiles, tiles,
            pltpu.VMEM((LEVELS * SUB, LANES), F32),
            pltpu.SemaphoreType.DMA((COPIES,)),
        ],
        compiler_params=params,
    )(*(pltpu.with_memory_space_constraint(x, pltpu.HBM) for x in (history, source, diffusivity, target)))
    got = lax.all_to_all(
        msg.reshape(BLOCKS, 4, LANES), AXIS, split_axis=0, concat_axis=0, tiled=True
    ).reshape(4 * BLOCKS, LANES)
    back = pl.pallas_call(
        reduced_kernel,
        name="reduced",
        out_shape=shape((BLOCKS, LANES), F32),
        in_specs=[vmem],
        out_specs=vmem,
        scratch_shapes=[pltpu.VMEM((BLOCKS + 2 * SUB, LANES), F32)] * 3,
        compiler_params=params,
    )(got)
    solved = lax.all_to_all(back, AXIS, split_axis=0, concat_axis=0, tiled=True)
    update, totals = pl.pallas_call(
        final_kernel,
        name="final",
        out_shape=[shape((VREGS * SUB, LANES), F32), shape((2,), F32)],
        in_specs=[vmem] * 4,
        out_specs=[vmem, pl.BlockSpec(memory_space=pltpu.SMEM)],
        compiler_params=params,
    )(solved, part, above, below)
    update = update.reshape(HALVES, TILES, SUB, LANES).transpose(0, 2, 1, 3).reshape(ROWS, NY)
    return update, totals


def solution(mesh):
    return jax.shard_map(
        body,
        mesh=mesh,
        in_specs=(P(None, AXIS, None), P(AXIS, None), P(AXIS, None), P(AXIS, None)),
        out_specs=(P(AXIS, None), P()),
        check_vma=False,
    )
```
